32 devices in a mesh: rows: 16 (over z, y, x), cent: 2 (over core).
Axes of the slice: x: 2, y: 2, z: 4, core: 2. Of those that a mesh axis runs over, the one named last changes fastest.
Arguments:
- points: bfloat16 [16384, 1024], P('rows'), may hold values from -8 to 8
- centroids: bfloat16 [4096, 1024], P('cent'), may hold values from -8 to 8
- assign: int32 [16384], P('rows'), may hold values from 0 to 4095, as said below
Outputs:
- nearest: float32 [2, 16384], P(None, 'rows')
- updated: bfloat16 [4096, 1024], P('cent')
The draws below stay inside these ranges and needn't reach their ends.
Inputs may be any that keep to these rules, and one draw needn't show every extreme that they name: `assign`: split the points into aligned blocks of 1024 and the centroids into aligned groups of 128 consecutive ones: in each block at most 64 points are assigned into any one group, and in every block some group takes exactly 64 of them.
All inputs are finite; a program needn't handle non-finite values.
Results may differ from the reference program's by a relative error of at most 0.001.
Values may be sent and summed in bfloat16 or wider, within the bound.
No kernel may reach another device: no remote copies, remote signals or barrier semaphores. Data moves between devices by JAX's collectives and lax.ppermute only.
A program may use at most 64 MiB of HBM per device.

```python
import jax
import jax.numpy as jnp
from jax import lax

D = 1024
K = 4096
PTS_DEV = 1024
P_SIZE = 16384
GROUPS = 32
SHARE = 128
CAP = 64


def centroid_field(key):
    key_dir, key_len = jax.random.split(jax.random.fold_in(key, 23), 2)
    raw = jax.random.normal(key_dir, (K, D), jnp.float32)
    length = jax.random.uniform(key_len, (K, 1), jnp.float32, 0.97, 1.03)
    return raw * (length * jnp.sqrt(jnp.float32(D)) / jnp.sqrt(jnp.sum(raw * raw, axis=1, keepdims=True)))


def draw_centroids(key, part):
    return centroid_field(key).astype(jnp.bfloat16)


def draw_points(key, part):
    key_val, key_scale, key_pick = jax.random.split(jax.random.fold_in(key, 37), 3)
    cents = centroid_field(key).astype(jnp.bfloat16).astype(jnp.float32)
    picks = jax.random.randint(key_pick, (P_SIZE,), 0, K)
    noise = jax.random.normal(key_val, (P_SIZE, D), jnp.float32)
    low, high = (0.2, 1.5)
    logs = jax.random.uniform(key_scale, (P_SIZE, 1), jnp.float32, jnp.log(low), jnp.log(high))
    scaled = jnp.clip(jnp.exp(logs) * cents[picks] + 0.3 * noise, -8.0, 8.0)
    return scaled.astype(jnp.bfloat16)


def draw_assign(key, part):
    blocks_total = P_SIZE // PTS_DEV
    key_block, key_order, key_shuffle, key_offset = jax.random.split(jax.random.fold_in(key, 11), 4)
    picked = jax.random.randint(key_block, (blocks_total,), 0, GROUPS)
    slot_group = jnp.repeat(jnp.arange(GROUPS, dtype=jnp.int32), CAP)

    def one_block(index):
        order = jax.random.permutation(jax.random.fold_in(key_order, index), GROUPS * CAP).astype(jnp.int32)
        forced = slot_group == picked[index]
        score = jnp.where(forced, order - GROUPS * CAP, order)
        chosen = slot_group[jnp.argsort(score, stable=True)[:PTS_DEV]]
        mixing = jax.random.permutation(jax.random.fold_in(key_shuffle, index), PTS_DEV)
        return chosen[mixing]
    groups_all = jax.vmap(one_block)(jnp.arange(blocks_total, dtype=jnp.int32))
    offsets = jax.random.randint(key_offset, (blocks_total, PTS_DEV), 0, SHARE)
    return (groups_all * SHARE + offsets).reshape(P_SIZE).astype(jnp.int32)


def setup_inputs(seed: int = 0) -> dict:
    arg_keys = jax.random.split(jax.random.key(seed), 4)
    return {
        "points": draw_points(jax.random.fold_in(arg_keys[3], 71), 0),
        "centroids": draw_centroids(jax.random.fold_in(arg_keys[3], 71), 0),
        "assign": draw_assign(jax.random.fold_in(arg_keys[3], 71), 0),
    }


def smallest(points, pnorm, cents):
    cnorm = jnp.sum(jnp.square(cents.astype(jnp.float32)), axis=1)
    size = P_SIZE
    if P_SIZE % 1024 == 0:
        size = 1024

    def one_block(pair):
        block, norms = pair
        dots = lax.dot_general(block, cents, (((1,), (1,)), ((), ())), preferred_element_type=jnp.float32)
        return jnp.min((norms[:, None] - 2.0 * dots + cnorm[None, :]) / D, axis=1)

    result = lax.map(one_block, (points.reshape(P_SIZE // size, size, D), pnorm.reshape(P_SIZE // size, size)))
    return result.reshape(P_SIZE)


def reference(points, centroids, assign):
    wide = points.astype(jnp.float32)
    pnorm = jnp.sum(jnp.square(wide), axis=1)
    first = smallest(points, pnorm, centroids)
    sums = jax.ops.segment_sum(wide, assign, num_segments=K)
    counts = jax.ops.segment_sum(jnp.ones((P_SIZE,), jnp.float32), assign, num_segments=K)
    updated = ((sums + centroids.astype(jnp.float32)) / (counts[:, None] + 1.0)).astype(jnp.bfloat16)
    second = smallest(points, pnorm, updated)
    return jnp.stack([first, second]), updated
```

```python
import jax
import jax.numpy as jnp
from jax import lax
from jax.sharding import PartitionSpec as P


def smallest(points, pnorm, cents):
    cnorm = jnp.sum(jnp.square(cents.astype(jnp.float32)), axis=1)
    dots = lax.dot_general(
        points, cents, (((1,), (1,)), ((), ())), preferred_element_type=jnp.float32
    )
    return jnp.min((pnorm[:, None] - 2.0 * dots + cnorm[None, :]) / points.shape[1], axis=1)


def swap(value, mask, axis="rows"):
    size = lax.axis_size(axis)
    return lax.ppermute(value, axis, [(i, i ^ mask) for i in range(size)])


def block_min(values):
    size = lax.axis_size("cent")
    if size & (size - 1):
        return lax.pmin(values, "cent")
    mask = 1
    while mask < size:
        values = jnp.minimum(values, swap(values, mask, "cent"))
        mask *= 2
    return values


def gather(piece):
    size = lax.axis_size("rows")
    if size < 4 or size & (size - 1):
        return lax.all_gather(piece, "rows", axis=0, tiled=True)
    me = lax.axis_index("rows")
    share, width = piece.shape
    half = share // 2
    parts = []
    columns = [piece] + [swap(piece, 4 * k) for k in range(1, size // 4)]
    for k, column in enumerate(columns):
        one, two = swap(column, 1), swap(column, 2)
        low, high = swap(two[:half], 1), swap(one[half:], 2)
        parts += [
            (4 * k, 0, column),
            (4 * k + 1, 0, one),
            (4 * k + 2, 0, two),
            (4 * k + 3, 0, low),
            (4 * k + 3, half, high),
        ]
    whole = jnp.zeros((size * share, width), piece.dtype)
    for mask, row, part in parts:
        whole = lax.dynamic_update_slice_in_dim(whole, part, (me ^ mask) * share + row, 0)
    return whole


def renew(part_sums, part_counts, own_rows):
    return ((part_sums + own_rows.astype(jnp.float32)) / (part_counts[:, None] + 1.0)).astype(
        jnp.bfloat16
    )


def per_device(points, centroids, assign):
    blocksize = centroids.shape[0]
    count_pts = points.shape[0]
    pnorm = jnp.sum(jnp.square(points.astype(jnp.float32)), axis=1)
    first = smallest(points, pnorm, centroids)
    relative = assign - lax.axis_index("cent") * blocksize
    share = blocksize // lax.axis_size("rows")
    own = lax.dynamic_slice_in_dim(centroids, lax.axis_index("rows") * share, share, 0)
    rows_count = lax.axis_size("rows")
    groups = rows_count * lax.axis_size("cent")
    capacity = max(2, 2 * count_pts // groups)
    inside = (relative >= 0) & (relative < blocksize)
    owners = jnp.where(inside, relative // share, rows_count)
    offsets = jnp.where(inside, relative - relative // share * share, 0)
    owner_hot = owners[:, None] == lax.broadcasted_iota(jnp.int32, (count_pts, rows_count), 1)
    earlier = lax.broadcasted_iota(jnp.int32, (count_pts, count_pts), 1) < lax.broadcasted_iota(
        jnp.int32, (count_pts, count_pts), 0
    )
    before = jnp.dot(
        earlier.astype(jnp.bfloat16),
        owner_hot.astype(jnp.bfloat16),
        preferred_element_type=jnp.float32,
    )
    ranking = jnp.sum(jnp.where(owner_hot, before, 0.0), axis=1).astype(jnp.int32)
    slot_index = jnp.where(inside, owners * capacity + ranking, -1)
    placing = (
        lax.broadcasted_iota(jnp.int32, (rows_count * capacity, count_pts), 0)
        == slot_index[None, :]
    )
    outgoing = jnp.dot(
        placing.astype(jnp.bfloat16), points, preferred_element_type=jnp.float32
    ).astype(jnp.bfloat16)
    labels = (jnp.sum(jnp.where(placing, offsets[None, :] + 1, 0), axis=1) - 1).astype(jnp.bfloat16)
    arrived, arrived_labels = (
        lax.all_to_all(outgoing, "rows", split_axis=0, concat_axis=0, tiled=True),
        lax.all_to_all(labels, "rows", split_axis=0, concat_axis=0, tiled=True),
    )
    first, arrived = lax.optimization_barrier((first, arrived))
    chosen = (
        lax.broadcasted_iota(jnp.int32, (share, arrived.shape[0]), 0)
        == arrived_labels.astype(jnp.int32)[None, :]
    )
    part_sums = jnp.dot(chosen.astype(jnp.bfloat16), arrived, preferred_element_type=jnp.float32)
    part_counts = jnp.sum(chosen.astype(jnp.float32), axis=1)
    updated = gather(renew(part_sums, part_counts, own))
    second = smallest(points, pnorm, updated)
    nearest = block_min(jnp.stack([first, second]))
    return (nearest, updated)


def solution(mesh):
    return jax.shard_map(
        per_device,
        mesh=mesh,
        in_specs=(P("rows", None), P("cent", None), P("rows")),
        out_specs=(P(None, "rows"), P("cent", None)),
        check_vma=False,
    )
```

```python
import functools

import jax
import jax.numpy as jnp
from jax import lax
from jax.experimental import pallas as pl
from jax.experimental.pallas import tpu as pltpu
from jax.sharding import PartitionSpec as P

F32 = jnp.float32
BF16 = jnp.bfloat16
VMEM = pl.BlockSpec(memory_space=pltpu.VMEM)
ANY = pl.BlockSpec(memory_space=pl.ANY)
LIMIT = 50 * 1024 * 1024
LABEL_ROWS = 8


def swap(value, mask, axis="rows"):
    size = lax.axis_size(axis)
    return lax.ppermute(value, axis, [(i, i ^ mask) for i in range(size)])


def block_min(values):
    size = lax.axis_size("cent")
    if size & (size - 1):
        return lax.pmin(values, "cent")
    mask = 1
    while mask < size:
        values = jnp.minimum(values, swap(values, mask, "cent"))
        mask *= 2
    return values


def cost(flops, moved):
    return pl.CostEstimate(flops=int(flops), bytes_accessed=int(moved), transcendentals=0)


def params():
    return pltpu.CompilerParams(vmem_limit_bytes=LIMIT)


def place_kernel(half, share, capacity, own, assign_ref, points_ref, *outs):
    me, cent = lax.axis_index("rows"), lax.axis_index("cent")
    count = assign_ref.shape[1]
    side = me // half if own else 1 - me // half
    owner = side * half + (
        lax.rem(me, half) ^ lax.broadcasted_iota(jnp.int32, (half, count), 0)
    )
    within = assign_ref[...] - (cent * 2 * half + owner) * share
    hot = (within >= 0) & (within < share)
    ones = jnp.where(hot, 1.0, 0.0).astype(F32)
    seg = 128
    upper = jnp.where(
        lax.broadcasted_iota(jnp.int32, (seg, seg), 0)
        < lax.broadcasted_iota(jnp.int32, (seg, seg), 1),
        1.0,
        0.0,
    ).astype(BF16)
    total = jnp.zeros((half, 1), F32)
    before = []
    for start in range(0, count, seg):
        piece = ones[:, start : start + seg]
        before.append(jnp.dot(piece.astype(BF16), upper, preferred_element_type=F32) + total)
        total = total + jnp.sum(piece, axis=1, keepdims=True)
    rank = jnp.where(hot, jnp.concatenate(before, axis=1), -1.0)
    label = jnp.sum(jnp.where(hot, within + 1, 0).astype(F32), axis=0, keepdims=True)
    label = jnp.transpose(jnp.broadcast_to(label, (8, count)))
    slots = lax.broadcasted_iota(jnp.int32, (capacity, count), 0).astype(F32)
    placing = jnp.concatenate(
        [jnp.where(slots == rank[m : m + 1], 1.0, 0.0).astype(BF16) for m in range(half)], axis=0
    )
    placed = jnp.dot(placing, points_ref[...], preferred_element_type=F32).astype(BF16)
    labels = jnp.dot(placing, label.astype(BF16), preferred_element_type=F32)
    labels = (jnp.transpose(labels) - 1.0).astype(BF16)
    for m in range(half):
        outs[m][:capacity, :] = placed[m * capacity : (m + 1) * capacity]
        outs[m][capacity:, :] = jnp.zeros((LABEL_ROWS, outs[m].shape[1]), BF16)
        outs[m][capacity:, :capacity] = labels[:, m * capacity : (m + 1) * capacity]


def place(own, points, assign_row, share, capacity):
    half = lax.axis_size("rows") // 2
    count, width = points.shape
    block = jax.ShapeDtypeStruct((capacity + LABEL_ROWS, width), BF16)
    return pl.pallas_call(
        functools.partial(place_kernel, half, share, capacity, own),
        out_shape=[block] * half,
        in_specs=[VMEM, VMEM],
        out_specs=[VMEM] * half,
        compiler_params=params(),
        cost_estimate=cost(2 * half * capacity * count * width, 4 * count * width),
        name="place_own" if own else "place_other",
    )(assign_row, points)


def sum_kernel(share, capacity, *refs):
    blocks, sums_ref, counts_ref = refs[:-2], refs[-2], refs[-1]
    labels = jnp.concatenate(
        [r[capacity:, :capacity].astype(F32)[:1] for r in blocks], axis=1
    )
    chosen = jnp.where(
        lax.broadcasted_iota(jnp.int32, (share, labels.shape[1]), 0).astype(F32) == labels, 1.0, 0.0
    ).astype(F32)
    rows = jnp.concatenate([r[:capacity, :] for r in blocks], axis=0)
    sums_ref[...] = jnp.dot(chosen.astype(BF16), rows, preferred_element_type=F32)
    counts = jnp.broadcast_to(jnp.sum(chosen, axis=1, keepdims=True), (share, 8))
    counts_ref[...] = jnp.transpose(counts)


def add_up(blocks, share, capacity, name):
    width = blocks[0].shape[1]
    return pl.pallas_call(
        functools.partial(sum_kernel, share, capacity),
        out_shape=[jax.ShapeDtypeStruct((share, width), F32), jax.ShapeDtypeStruct((8, share), F32)],
        in_specs=[VMEM] * len(blocks),
        out_specs=[VMEM, VMEM],
        compiler_params=params(),
        cost_estimate=cost(2 * share * len(blocks) * capacity * width, 3 * share * width * 4),
        name=name,
    )(*blocks)


def renew_kernel(sums_ref, counts_ref, far_sums_ref, far_counts_ref, own_ref, out_ref):
    counts = jnp.transpose(counts_ref[...] + far_counts_ref[...])[:, :1]
    total = sums_ref[...] + far_sums_ref[...] + own_ref[...].astype(F32)
    out_ref[...] = (total / (counts + 1.0)).astype(BF16)


def renew(sums, counts, far_sums, far_counts, own):
    return pl.pallas_call(
        renew_kernel,
        out_shape=jax.ShapeDtypeStruct(own.shape, BF16),
        in_specs=[VMEM] * 5,
        out_specs=VMEM,
        compiler_params=params(),
        cost_estimate=cost(4 * own.size, 14 * own.size),
        name="renew",
    )(sums, counts, far_sums, far_counts, own)


def lowest(cents, columns):
    wide = cents.astype(F32)
    norms = jnp.sum(wide * wide, axis=1, keepdims=True)
    scores = norms - 2.0 * jnp.dot(cents, columns, preferred_element_type=F32)
    return jnp.min(scores.reshape(-1, 8, scores.shape[1]), axis=0)


def first_kernel(step, cents_ref, columns_ref, out_ref):
    out_ref[...] = jnp.full(out_ref.shape, jnp.inf, F32)

    @pl.loop(0, cents_ref.shape[0] // step)
    def _(i):
        start = pl.multiple_of(i * step, step)
        out_ref[...] = jnp.minimum(
            out_ref[...], lowest(cents_ref[pl.ds(start, step), :], columns_ref[...])
        )


def first_lowest(cents, columns):
    return pl.pallas_call(
        functools.partial(first_kernel, 256),
        out_shape=jax.ShapeDtypeStruct((8, columns.shape[1]), F32),
        in_specs=[VMEM, VMEM],
        out_specs=VMEM,
        compiler_params=params(),
        cost_estimate=cost(2 * cents.size * columns.shape[1], 2 * cents.size),
        name="first_lowest",
    )(cents, columns)


def arrive_kernel(share, places, fresh, *refs):
    count = len(places)
    pieces, columns_ref = refs[:count], refs[count]
    rest = refs[count + 1 :] if fresh else refs[count + 3 :]
    running_out, whole_out, sems = rest
    me = lax.axis_index("rows")
    copies = []
    for i, (masks, ref) in enumerate(zip(places, pieces, strict=True)):
        for j, mask in enumerate(masks):
            copy = pltpu.make_async_copy(
                ref.at[pl.ds(j * share, share)],
                whole_out.at[pl.ds(pl.multiple_of((me ^ mask) * share, share), share)],
                sems.at[len(copies)],
            )
            copy.start()
            copies.append(copy)
    found = lowest(jnp.concatenate([r[...] for r in pieces], axis=0), columns_ref[...])
    running_out[...] = found if fresh else jnp.minimum(refs[count + 1][...], found)
    for copy in copies:
        copy.wait()


def arrive(pieces, columns, running, whole, total, name):
    places = [masks for masks, _ in pieces]
    share = pieces[0][1].shape[0] // len(places[0])
    width = pieces[0][1].shape[1]
    fresh = running is None
    rows = share * sum(len(m) for m in places)
    operands = [array for _, array in pieces] + [columns]
    specs = [VMEM] * len(operands)
    aliases = {}
    if not fresh:
        aliases = {len(operands) + 1: 1}
        operands += [running, whole]
        specs += [VMEM, ANY]
    return pl.pallas_call(
        functools.partial(arrive_kernel, share, places, fresh),
        out_shape=[
            jax.ShapeDtypeStruct((8, columns.shape[1]), F32),
            jax.ShapeDtypeStruct((total, width), BF16),
        ],
        in_specs=specs,
        out_specs=[VMEM, ANY],
        scratch_shapes=[pltpu.SemaphoreType.DMA((sum(len(m) for m in places),))],
        input_output_aliases=aliases,
        compiler_params=params(),
        cost_estimate=cost(2 * rows * width * columns.shape[1], 4 * rows * width),
        name=name,
    )(*operands)


def halves(points, centroids, assign, share, capacity):
    rows_count = lax.axis_size("rows")
    half = rows_count // 2
    me = lax.axis_index("rows")
    own = lax.dynamic_slice_in_dim(centroids, me * share, share, 0)
    assign_row = assign.reshape(1, -1)

    with jax.named_scope("far_points"):
        far = place(False, points, assign_row, share, capacity)
        far = [far[0]] + [swap(far[m], m) for m in range(1, half)]
    columns = jnp.transpose(points)
    near = place(True, points, assign_row, share, capacity)
    far_sums, far_counts = add_up(far, share, capacity, "far_sum")
    far_sums, far_counts, near = lax.optimization_barrier((far_sums, far_counts, near))
    with jax.named_scope("far_sums"):
        far_sums = swap(far_sums, half)
    with jax.named_scope("far_counts"):
        far_counts = swap(far_counts, half)
    with jax.named_scope("near_points"):
        near = [near[0]] + [swap(near[m], m) for m in range(1, half)]
    first = first_lowest(centroids, columns)
    near_sums, near_counts = add_up(near, share, capacity, "near_sum")
    first, far_sums = lax.optimization_barrier((first, far_sums))
    piece = renew(near_sums, near_counts, far_sums, far_counts, own)

    pieces = [piece] + [swap(piece, 4 * k) for k in range(1, rows_count // 4)]
    running, whole = None, None
    for k in range(0, rows_count // 4, 2):
        one, two = pieces[k], pieces[k + 1]
        one_x, two_y = swap(one, 1), swap(two, 2)
        pair_y = swap(jnp.concatenate([one, one_x], axis=0), 2)
        pair_x = swap(jnp.concatenate([two, two_y], axis=0), 1)
        m, n = 4 * k, 4 * (k + 1)
        first_part = [((m,), one), ((m ^ 1,), one_x), ((n,), two), ((n ^ 2,), two_y)]
        running, whole = arrive(
            first_part, columns, running, whole, rows_count * share, f"arrive_{k}"
        )
        last_part = [((m ^ 2, m ^ 3), pair_y), ((n ^ 1, n ^ 3), pair_x)]
        running, whole = arrive(
            last_part, columns, running, whole, rows_count * share, f"arrive_{k + 1}"
        )
    pnorm = jnp.sum(jnp.square(points.astype(F32)), axis=1)
    both = jnp.stack([jnp.min(first, axis=0), jnp.min(running, axis=0)])
    nearest = block_min((pnorm[None, :] + both) / points.shape[1])
    return nearest, whole


def smallest(points, pnorm, cents):
    cnorm = jnp.sum(jnp.square(cents.astype(F32)), axis=1)
    dots = lax.dot_general(points, cents, (((1,), (1,)), ((), ())), preferred_element_type=F32)
    return jnp.min((pnorm[:, None] - 2.0 * dots + cnorm[None, :]) / points.shape[1], axis=1)


def plain(points, centroids, assign, share, capacity):
    blocksize = centroids.shape[0]
    count_pts = points.shape[0]
    pnorm = jnp.sum(jnp.square(points.astype(F32)), axis=1)
    first = smallest(points, pnorm, centroids)
    relative = assign - lax.axis_index("cent") * blocksize
    own = lax.dynamic_slice_in_dim(centroids, lax.axis_index("rows") * share, share, 0)
    rows_count = lax.axis_size("rows")
    inside = (relative >= 0) & (relative < blocksize)
    owners = jnp.where(inside, relative // share, rows_count)
    offsets = jnp.where(inside, relative - relative // share * share, 0)
    owner_hot = owners[:, None] == lax.broadcasted_iota(jnp.int32, (count_pts, rows_count), 1)
    earlier = lax.broadcasted_iota(jnp.int32, (count_pts, count_pts), 1) < lax.broadcasted_iota(
        jnp.int32, (count_pts, count_pts), 0
    )
    before = jnp.dot(earlier.astype(BF16), owner_hot.astype(BF16), preferred_element_type=F32)
    ranking = jnp.sum(jnp.where(owner_hot, before, 0.0), axis=1).astype(jnp.int32)
    slot_index = jnp.where(inside, owners * capacity + ranking, -1)
    placing = (
        lax.broadcasted_iota(jnp.int32, (rows_count * capacity, count_pts), 0)
        == slot_index[None, :]
    )
    outgoing = jnp.dot(placing.astype(BF16), points, preferred_element_type=F32).astype(BF16)
    labels = (jnp.sum(jnp.where(placing, offsets[None, :] + 1, 0), axis=1) - 1).astype(BF16)
    arrived = lax.all_to_all(outgoing, "rows", split_axis=0, concat_axis=0, tiled=True)
    arrived_labels = lax.all_to_all(labels, "rows", split_axis=0, concat_axis=0, tiled=True)
    chosen = (
        lax.broadcasted_iota(jnp.int32, (share, arrived.shape[0]), 0)
        == arrived_labels.astype(jnp.int32)[None, :]
    )
    sums = jnp.dot(chosen.astype(BF16), arrived, preferred_element_type=F32)
    counts = jnp.sum(chosen.astype(F32), axis=1)
    piece = ((sums + own.astype(F32)) / (counts[:, None] + 1.0)).astype(BF16)
    updated = lax.all_gather(piece, "rows", axis=0, tiled=True)
    second = smallest(points, pnorm, updated)
    return block_min(jnp.stack([first, second])), updated


def per_device(points, centroids, assign):
    rows_count = lax.axis_size("rows")
    share = centroids.shape[0] // rows_count
    groups = rows_count * lax.axis_size("cent")
    capacity = max(2, 2 * points.shape[0] // groups)
    fits = (
        rows_count >= 8
        and rows_count & (rows_count - 1) == 0
        and share % 128 == 0
        and share <= 256
        and capacity % 16 == 0
        and points.shape[0] % 128 == 0
        and points.shape[1] % 128 == 0
        and centroids.shape[0] % 256 == 0
    )
    return (halves if fits else plain)(points, centroids, assign, share, capacity)


def solution(mesh):
    return jax.shard_map(
        per_device,
        mesh=mesh,
        in_specs=(P("rows", None), P("cent", None), P("rows")),
        out_specs=(P(None, "rows"), P("cent", None)),
        check_vma=False,
    )
```

```python
import functools

import jax
import jax.numpy as jnp
from jax import lax
from jax.experimental import pallas as pl
from jax.experimental.pallas import tpu as pltpu
from jax.sharding import PartitionSpec as P


F32 = jnp.float32
BF16 = jnp.bfloat16
VMEM = pl.BlockSpec(memory_space=pltpu.VMEM)
ANY = pl.BlockSpec(memory_space=pl.ANY)
HBM = pl.BlockSpec(memory_space=pltpu.HBM)
LIMIT = 24 * 1024 * 1024
LABEL_ROWS = 8


def swap(value, mask, axis="rows"):
    size = lax.axis_size(axis)
    return lax.ppermute(value, axis, [(i, i ^ mask) for i in range(size)])


def block_min(values):
    size = lax.axis_size("cent")
    if size & (size - 1):
        return lax.pmin(values, "cent")
    mask = 1
    while mask < size:
        values = jnp.minimum(values, swap(values, mask, "cent"))
        mask *= 2
    return values


def cost(flops, moved):
    return pl.CostEstimate(flops=int(flops), bytes_accessed=int(moved), transcendentals=0)


def params():
    return pltpu.CompilerParams(vmem_limit_bytes=LIMIT)


def place_kernel(half, share, capacity, own, assign_ref, points_hbm, *refs):
    outs, (points_ref, sem) = refs[:-2], refs[-2:]
    copy = pltpu.make_async_copy(points_hbm, points_ref, sem)
    copy.start()
    me, cent = lax.axis_index("rows"), lax.axis_index("cent")
    count = assign_ref.shape[1]
    side = me // half if own else 1 - me // half
    owner = side * half + (
        lax.rem(me, half) ^ lax.broadcasted_iota(jnp.int32, (half, count), 0)
    )
    within = assign_ref[...] - (cent * 2 * half + owner) * share
    hot = (within >= 0) & (within < share)
    ones = jnp.where(hot, 1.0, 0.0).astype(F32)
    seg = 128
    upper = jnp.where(
        lax.broadcasted_iota(jnp.int32, (seg, seg), 0)
        < lax.broadcasted_iota(jnp.int32, (seg, seg), 1),
        1.0,
        0.0,
    ).astype(BF16)
    total = jnp.zeros((half, 1), F32)
    before = []
    for start in range(0, count, seg):
        piece = ones[:, start : start + seg]
        before.append(jnp.dot(piece.astype(BF16), upper, preferred_element_type=F32) + total)
        total = total + jnp.sum(piece, axis=1, keepdims=True)
    rank = jnp.where(hot, jnp.concatenate(before, axis=1), -1.0)
    label = jnp.sum(jnp.where(hot, within + 1, 0).astype(F32), axis=0, keepdims=True)
    label = jnp.transpose(jnp.broadcast_to(label, (8, count)))
    slots = lax.broadcasted_iota(jnp.int32, (capacity, count), 0).astype(F32)
    placing = jnp.concatenate(
        [jnp.where(slots == rank[m : m + 1], 1.0, 0.0).astype(BF16) for m in range(half)], axis=0
    )
    copy.wait()
    placed = jnp.dot(placing, points_ref[...], preferred_element_type=F32).astype(BF16)
    labels = jnp.dot(placing, label.astype(BF16), preferred_element_type=F32)
    labels = (jnp.transpose(labels) - 1.0).astype(BF16)
    for m in range(half):
        outs[m][:capacity, :] = placed[m * capacity : (m + 1) * capacity]
        outs[m][capacity:, :] = jnp.zeros((LABEL_ROWS, outs[m].shape[1]), BF16)
        outs[m][capacity:, :capacity] = labels[:, m * capacity : (m + 1) * capacity]


def place(own, points, assign_row, share, capacity):
    half = lax.axis_size("rows") // 2
    count, width = points.shape
    block = jax.ShapeDtypeStruct((capacity + LABEL_ROWS, width), BF16)
    return pl.pallas_call(
        functools.partial(place_kernel, half, share, capacity, own),
        out_shape=[block] * half,
        in_specs=[VMEM, HBM],
        out_specs=[VMEM] * half,
        scratch_shapes=[pltpu.VMEM((count, width), BF16), pltpu.SemaphoreType.DMA],
        compiler_params=params(),
        cost_estimate=cost(2 * half * capacity * count * width, 4 * count * width),
        name="place_own" if own else "place_other",
    )(assign_row, points)


def sum_kernel(share, capacity, *refs):
    blocks, sums_ref, counts_ref = refs[:-2], refs[-2], refs[-1]
    labels = jnp.concatenate(
        [r[capacity:, :capacity].astype(F32)[:1] for r in blocks], axis=1
    )
    chosen = jnp.where(
        lax.broadcasted_iota(jnp.int32, (share, labels.shape[1]), 0).astype(F32) == labels, 1.0, 0.0
    ).astype(F32)
    rows = jnp.concatenate([r[:capacity, :] for r in blocks], axis=0)
    sums_ref[...] = jnp.dot(chosen.astype(BF16), rows, preferred_element_type=F32)
    counts = jnp.broadcast_to(jnp.sum(chosen, axis=1, keepdims=True), (share, 8))
    counts_ref[...] = jnp.transpose(counts)


def add_up(blocks, share, capacity):
    width = blocks[0].shape[1]
    return pl.pallas_call(
        functools.partial(sum_kernel, share, capacity),
        out_shape=[jax.ShapeDtypeStruct((share, width), F32), jax.ShapeDtypeStruct((8, share), F32)],
        in_specs=[VMEM] * len(blocks),
        out_specs=[VMEM, VMEM],
        compiler_params=params(),
        cost_estimate=cost(2 * share * len(blocks) * capacity * width, 3 * share * width * 4),
    )(*blocks)


def renew_kernel(sums_ref, counts_ref, far_sums_ref, far_counts_ref, own_ref, out_ref):
    counts = jnp.transpose(counts_ref[...] + far_counts_ref[...])[:, :1]
    total = sums_ref[...] + far_sums_ref[...] + own_ref[...].astype(F32)
    out_ref[...] = (total / (counts + 1.0)).astype(BF16)


def renew(sums, counts, far_sums, far_counts, own):
    return pl.pallas_call(
        renew_kernel,
        out_shape=jax.ShapeDtypeStruct(own.shape, BF16),
        in_specs=[VMEM] * 5,
        out_specs=VMEM,
        compiler_params=params(),
        cost_estimate=cost(4 * own.size, 14 * own.size),
        name="renew",
    )(sums, counts, far_sums, far_counts, own)


def lowest(cents, columns):
    wide = cents.astype(F32)
    norms = jnp.sum(wide * wide, axis=1, keepdims=True)
    scores = norms - 2.0 * jnp.dot(cents, columns, preferred_element_type=F32)
    return jnp.min(scores.reshape(-1, 8, scores.shape[1]), axis=0)


def first_kernel(step, cents_ref, columns_ref, out_ref):
    out_ref[...] = jnp.full(out_ref.shape, jnp.inf, F32)

    @pl.loop(0, cents_ref.shape[0] // step)
    def _(i):
        start = pl.multiple_of(i * step, step)
        out_ref[...] = jnp.minimum(
            out_ref[...], lowest(cents_ref[pl.ds(start, step), :], columns_ref[...])
        )


def first_lowest(cents, columns):
    return pl.pallas_call(
        functools.partial(first_kernel, 256),
        out_shape=jax.ShapeDtypeStruct((8, columns.shape[1]), F32),
        in_specs=[VMEM, VMEM],
        out_specs=VMEM,
        compiler_params=params(),
        cost_estimate=cost(2 * cents.size * columns.shape[1], 2 * cents.size),
        name="first_lowest",
    )(cents, columns)


def arrive_kernel(share, places, fresh, *refs):
    count = len(places)
    pieces, columns_ref = refs[:count], refs[count]
    rest = refs[count + 1 :] if fresh else refs[count + 3 :]
    running_out, whole_out, sems = rest
    me = lax.axis_index("rows")
    copies = []
    for i, ((mask, row), ref) in enumerate(zip(places, pieces, strict=True)):
        start = pl.multiple_of((me ^ mask) * share + row, ref.shape[0])
        copy = pltpu.make_async_copy(
            ref, whole_out.at[pl.ds(start, ref.shape[0])], sems.at[i]
        )
        copy.start()
        copies.append(copy)
    found = lowest(jnp.concatenate([r[...] for r in pieces], axis=0), columns_ref[...])
    running_out[...] = found if fresh else jnp.minimum(refs[count + 1][...], found)
    for copy in copies:
        copy.wait()


def arrive(pieces, columns, running, whole, total, share):
    places = [(mask, row) for mask, row, _ in pieces]
    operands = [array for _, _, array in pieces]
    rows, width = sum(o.shape[0] for o in operands), operands[0].shape[1]
    fresh = running is None
    operands += [columns]
    specs = [VMEM] * len(operands)
    aliases = {}
    if not fresh:
        aliases = {len(operands) + 1: 1}
        operands += [running, whole]
        specs += [VMEM, ANY]
    return pl.pallas_call(
        functools.partial(arrive_kernel, share, places, fresh),
        out_shape=[
            jax.ShapeDtypeStruct((8, columns.shape[1]), F32),
            jax.ShapeDtypeStruct((total, width), BF16),
        ],
        in_specs=specs,
        out_specs=[VMEM, ANY],
        scratch_shapes=[pltpu.SemaphoreType.DMA((len(places),))],
        input_output_aliases=aliases,
        compiler_params=params(),
        cost_estimate=cost(2 * rows * width * columns.shape[1], 4 * rows * width),
    )(*operands)


def halves(points, centroids, assign, share, capacity):
    rows_count = lax.axis_size("rows")
    half = rows_count // 2
    me = lax.axis_index("rows")
    total = rows_count * share
    own = lax.dynamic_slice_in_dim(centroids, me * share, share, 0)
    assign_row = assign.reshape(1, -1)

    far = place(False, points, assign_row, share, capacity)
    far = [far[0]] + [swap(far[m], m) for m in range(1, half)]
    near = place(True, points, assign_row, share, capacity)
    near = [near[0]] + [swap(near[m], m) for m in range(1, half)]
    far_sums, far_counts = add_up(far, share, capacity)
    far_sums, late = lax.optimization_barrier((far_sums, points))
    far_sums = swap(far_sums, half)
    far_counts = swap(far_counts, half)
    columns = jnp.transpose(late)
    first = first_lowest(centroids, columns)
    near_sums, near_counts = add_up(near, share, capacity)
    pnorm = jnp.sum(jnp.square(late.astype(F32)), axis=1)
    first, pnorm, own, far_sums = lax.optimization_barrier((first, pnorm, own, far_sums))
    piece = renew(near_sums, near_counts, far_sums, far_counts, own)

    cut = share // 2
    running, whole = None, None
    columns_count = rows_count // 4
    for k in range(columns_count):
        one = piece if k == 0 else swap(piece, 4 * k)
        one_x, one_y = swap(one, 1), swap(one, 2)
        low = swap(one_y[:cut], 1)
        high = swap(one_x[cut:], 2)
        m = 4 * k
        sides = [(m, 0, one), (m ^ 1, 0, one_x), (m ^ 2, 0, one_y)]
        corner = [(m ^ 3, 0, low), (m ^ 3, cut, high)]
        if k == columns_count - 1:
            running, whole = arrive(sides, columns, running, whole, total, share)
            running, whole = arrive(corner, columns, running, whole, total, share)
        else:
            running, whole = arrive(sides + corner, columns, running, whole, total, share)
    both = jnp.stack([jnp.min(first, axis=0), jnp.min(running, axis=0)])
    nearest = block_min((pnorm[None, :] + both) / points.shape[1])
    return nearest, whole


def smallest(points, pnorm, cents):
    cnorm = jnp.sum(jnp.square(cents.astype(F32)), axis=1)
    dots = lax.dot_general(points, cents, (((1,), (1,)), ((), ())), preferred_element_type=F32)
    return jnp.min((pnorm[:, None] - 2.0 * dots + cnorm[None, :]) / points.shape[1], axis=1)


def plain(points, centroids, assign, share, capacity):
    blocksize = centroids.shape[0]
    count_pts = points.shape[0]
    pnorm = jnp.sum(jnp.square(points.astype(F32)), axis=1)
    first = smallest(points, pnorm, centroids)
    relative = assign - lax.axis_index("cent") * blocksize
    own = lax.dynamic_slice_in_dim(centroids, lax.axis_index("rows") * share, share, 0)
    rows_count = lax.axis_size("rows")
    inside = (relative >= 0) & (relative < blocksize)
    owners = jnp.where(inside, relative // share, rows_count)
    offsets = jnp.where(inside, relative - relative // share * share, 0)
    owner_hot = owners[:, None] == lax.broadcasted_iota(jnp.int32, (count_pts, rows_count), 1)
    earlier = lax.broadcasted_iota(jnp.int32, (count_pts, count_pts), 1) < lax.broadcasted_iota(
        jnp.int32, (count_pts, count_pts), 0
    )
    before = jnp.dot(earlier.astype(BF16), owner_hot.astype(BF16), preferred_element_type=F32)
    ranking = jnp.sum(jnp.where(owner_hot, before, 0.0), axis=1).astype(jnp.int32)
    slot_index = jnp.where(inside, owners * capacity + ranking, -1)
    placing = (
        lax.broadcasted_iota(jnp.int32, (rows_count * capacity, count_pts), 0)
        == slot_index[None, :]
    )
    outgoing = jnp.dot(placing.astype(BF16), points, preferred_element_type=F32).astype(BF16)
    labels = (jnp.sum(jnp.where(placing, offsets[None, :] + 1, 0), axis=1) - 1).astype(BF16)
    arrived = lax.all_to_all(outgoing, "rows", split_axis=0, concat_axis=0, tiled=True)
    arrived_labels = lax.all_to_all(labels, "rows", split_axis=0, concat_axis=0, tiled=True)
    chosen = (
        lax.broadcasted_iota(jnp.int32, (share, arrived.shape[0]), 0)
        == arrived_labels.astype(jnp.int32)[None, :]
    )
    sums = jnp.dot(chosen.astype(BF16), arrived, preferred_element_type=F32)
    counts = jnp.sum(chosen.astype(F32), axis=1)
    piece = ((sums + own.astype(F32)) / (counts[:, None] + 1.0)).astype(BF16)
    updated = lax.all_gather(piece, "rows", axis=0, tiled=True)
    second = smallest(points, pnorm, updated)
    return block_min(jnp.stack([first, second])), updated


def fits(rows_count, share, capacity, count, width, blocksize):
    return (
        rows_count >= 8
        and rows_count & (rows_count - 1) == 0
        and share % 128 == 0
        and share <= 256
        and capacity % 16 == 0
        and count % 128 == 0
        and width % 128 == 0
        and blocksize % 256 == 0
    )


def per_device(points, centroids, assign):
    rows_count = lax.axis_size("rows")
    share = centroids.shape[0] // rows_count
    groups = rows_count * lax.axis_size("cent")
    capacity = max(2, 2 * points.shape[0] // groups)
    good = fits(rows_count, share, capacity, *points.shape, centroids.shape[0])
    if not good:
        return plain(points, centroids, assign, share, capacity)
    return halves(points, centroids, assign, share, capacity)


def solution(mesh):
    return jax.shard_map(
        per_device,
        mesh=mesh,
        in_specs=(P("rows", None), P("cent", None), P("rows")),
        out_specs=(P(None, "rows"), P("cent", None)),
        check_vma=False,
    )
```

```python
import functools

import jax
import jax.numpy as jnp
from jax import lax
from jax.experimental import pallas as pl
from jax.experimental.pallas import tpu as pltpu
from jax.sharding import PartitionSpec as P


F32 = jnp.float32
BF16 = jnp.bfloat16
VMEM = pl.BlockSpec(memory_space=pltpu.VMEM)
ANY = pl.BlockSpec(memory_space=pl.ANY)
HBM = pl.BlockSpec(memory_space=pltpu.HBM)
LIMIT = 24 * 1024 * 1024
LABEL_ROWS = 8


def swap(value, mask, axis="rows"):
    size = lax.axis_size(axis)
    return lax.ppermute(value, axis, [(i, i ^ mask) for i in range(size)])


def block_min(values):
    size = lax.axis_size("cent")
    if size & (size - 1):
        return lax.pmin(values, "cent")
    mask = 1
    while mask < size:
        values = jnp.minimum(values, swap(values, mask, "cent"))
        mask *= 2
    return values


def cost(flops, moved):
    return pl.CostEstimate(flops=int(flops), bytes_accessed=int(moved), transcendentals=0)


def params():
    return pltpu.CompilerParams(vmem_limit_bytes=LIMIT)


def rank_kernel(half, share, assign_ref, far_ref, near_ref, far_label_ref, near_label_ref):
    me, cent = lax.axis_index("rows"), lax.axis_index("cent")
    count = assign_ref.shape[1]
    seg = 128
    upper = jnp.where(
        lax.broadcasted_iota(jnp.int32, (seg, seg), 0)
        < lax.broadcasted_iota(jnp.int32, (seg, seg), 1),
        1.0,
        0.0,
    ).astype(BF16)
    low = lax.rem(me, half) ^ lax.broadcasted_iota(jnp.int32, (half, count), 0)
    for side, rank_ref, label_ref in (
        (1 - me // half, far_ref, far_label_ref),
        (me // half, near_ref, near_label_ref),
    ):
        within = assign_ref[...] - (cent * 2 * half + side * half + low) * share
        hot = (within >= 0) & (within < share)
        ones = jnp.where(hot, 1.0, 0.0).astype(F32)
        total = jnp.zeros((half, 1), F32)
        before = []
        for start in range(0, count, seg):
            piece = ones[:, start : start + seg]
            before.append(jnp.dot(piece.astype(BF16), upper, preferred_element_type=F32) + total)
            total = total + jnp.sum(piece, axis=1, keepdims=True)
        rank_ref[...] = jnp.where(hot, jnp.concatenate(before, axis=1), -1.0)
        label = jnp.sum(jnp.where(hot, within + 1, 0).astype(F32), axis=0, keepdims=True)
        label_ref[...] = jnp.transpose(jnp.broadcast_to(label, (8, count))).astype(BF16)


def ranks(assign_row, half, share):
    count = assign_row.shape[1]
    rank = jax.ShapeDtypeStruct((half, count), F32)
    label = jax.ShapeDtypeStruct((count, 8), BF16)
    return pl.pallas_call(
        functools.partial(rank_kernel, half, share),
        out_shape=[rank, rank, label, label],
        in_specs=[VMEM],
        out_specs=[VMEM] * 4,
        compiler_params=params(),
        cost_estimate=cost(4 * half * count * 128, 64 * count),
        name="ranks",
    )(assign_row)


def place_kernel(half, capacity, rank_ref, label_ref, points_ref, *outs):
    count = points_ref.shape[0]
    slots = lax.broadcasted_iota(jnp.int32, (capacity, count), 0).astype(F32)
    placing = jnp.concatenate(
        [
            jnp.where(slots == rank_ref[m : m + 1, :], 1.0, 0.0).astype(BF16)
            for m in range(half)
        ],
        axis=0,
    )
    placed = jnp.dot(placing, points_ref[...], preferred_element_type=F32).astype(BF16)
    labels = jnp.dot(placing, label_ref[...], preferred_element_type=F32)
    labels = (jnp.transpose(labels) - 1.0).astype(BF16)
    for m in range(half):
        outs[m][:capacity, :] = placed[m * capacity : (m + 1) * capacity]
        outs[m][capacity:, :] = jnp.zeros((LABEL_ROWS, outs[m].shape[1]), BF16)
        outs[m][capacity:, :capacity] = labels[:, m * capacity : (m + 1) * capacity]


def place(rank, label, points, capacity):
    half = rank.shape[0]
    count, width = points.shape
    block = jax.ShapeDtypeStruct((capacity + LABEL_ROWS, width), BF16)
    return pl.pallas_call(
        functools.partial(place_kernel, half, capacity),
        out_shape=[block] * half,
        in_specs=[VMEM] * 3,
        out_specs=[VMEM] * half,
        compiler_params=params(),
        cost_estimate=cost(2 * half * capacity * count * width, 4 * count * width),
    )(rank, label, points)


def sum_kernel(share, capacity, *refs):
    blocks, sums_ref, counts_ref = refs[:-2], refs[-2], refs[-1]
    labels = jnp.concatenate(
        [r[capacity:, :capacity].astype(F32)[:1] for r in blocks], axis=1
    )
    chosen = jnp.where(
        lax.broadcasted_iota(jnp.int32, (share, labels.shape[1]), 0).astype(F32) == labels, 1.0, 0.0
    ).astype(F32)
    rows = jnp.concatenate([r[:capacity, :] for r in blocks], axis=0)
    sums_ref[...] = jnp.dot(chosen.astype(BF16), rows, preferred_element_type=F32)
    counts = jnp.broadcast_to(jnp.sum(chosen, axis=1, keepdims=True), (share, 8))
    counts_ref[...] = jnp.transpose(counts)


def add_up(blocks, share, capacity):
    width = blocks[0].shape[1]
    return pl.pallas_call(
        functools.partial(sum_kernel, share, capacity),
        out_shape=[jax.ShapeDtypeStruct((share, width), F32), jax.ShapeDtypeStruct((8, share), F32)],
        in_specs=[VMEM] * len(blocks),
        out_specs=[VMEM, VMEM],
        compiler_params=params(),
        cost_estimate=cost(2 * share * len(blocks) * capacity * width, 3 * share * width * 4),
    )(*blocks)


def renew_kernel(sums_ref, counts_ref, far_sums_ref, far_counts_ref, own_ref, out_ref):
    counts = jnp.transpose(counts_ref[...] + far_counts_ref[...])[:, :1]
    total = sums_ref[...] + far_sums_ref[...] + own_ref[...].astype(F32)
    out_ref[...] = (total / (counts + 1.0)).astype(BF16)


def renew(sums, counts, far_sums, far_counts, own):
    return pl.pallas_call(
        renew_kernel,
        out_shape=jax.ShapeDtypeStruct(own.shape, BF16),
        in_specs=[VMEM] * 5,
        out_specs=VMEM,
        compiler_params=params(),
        cost_estimate=cost(4 * own.size, 14 * own.size),
        name="renew",
    )(sums, counts, far_sums, far_counts, own)


def lowest(cents, columns):
    wide = cents.astype(F32)
    norms = jnp.sum(wide * wide, axis=1, keepdims=True)
    scores = norms - 2.0 * jnp.dot(cents, columns, preferred_element_type=F32)
    return jnp.min(scores.reshape(-1, 8, scores.shape[1]), axis=0)


def first_kernel(step, cents_ref, columns_ref, out_ref):
    out_ref[...] = jnp.full(out_ref.shape, jnp.inf, F32)

    @pl.loop(0, cents_ref.shape[0] // step)
    def _(i):
        start = pl.multiple_of(i * step, step)
        out_ref[...] = jnp.minimum(
            out_ref[...], lowest(cents_ref[pl.ds(start, step), :], columns_ref[...])
        )


def first_lowest(cents, columns):
    return pl.pallas_call(
        functools.partial(first_kernel, 256),
        out_shape=jax.ShapeDtypeStruct((8, columns.shape[1]), F32),
        in_specs=[VMEM, VMEM],
        out_specs=VMEM,
        compiler_params=params(),
        cost_estimate=cost(2 * cents.size * columns.shape[1], 2 * cents.size),
        name="first_lowest",
    )(cents, columns)


def arrive_kernel(share, places, fresh, *refs):
    count = len(places)
    pieces, columns_ref = refs[:count], refs[count]
    rest = refs[count + 1 :] if fresh else refs[count + 3 :]
    running_out, whole_out, sems = rest
    me = lax.axis_index("rows")
    copies = []
    for i, ((mask, row), ref) in enumerate(zip(places, pieces, strict=True)):
        start = pl.multiple_of((me ^ mask) * share + row, ref.shape[0])
        copy = pltpu.make_async_copy(
            ref, whole_out.at[pl.ds(start, ref.shape[0])], sems.at[i]
        )
        copy.start()
        copies.append(copy)
    found = lowest(jnp.concatenate([r[...] for r in pieces], axis=0), columns_ref[...])
    running_out[...] = found if fresh else jnp.minimum(refs[count + 1][...], found)
    for copy in copies:
        copy.wait()


def arrive(pieces, columns, running, whole, total, share):
    places = [(mask, row) for mask, row, _ in pieces]
    operands = [array for _, _, array in pieces]
    rows, width = sum(o.shape[0] for o in operands), operands[0].shape[1]
    fresh = running is None
    operands += [columns]
    specs = [VMEM] * len(operands)
    aliases = {}
    if not fresh:
        aliases = {len(operands) + 1: 1}
        operands += [running, whole]
        specs += [VMEM, ANY]
    return pl.pallas_call(
        functools.partial(arrive_kernel, share, places, fresh),
        out_shape=[
            jax.ShapeDtypeStruct((8, columns.shape[1]), F32),
            jax.ShapeDtypeStruct((total, width), BF16),
        ],
        in_specs=specs,
        out_specs=[VMEM, ANY],
        scratch_shapes=[pltpu.SemaphoreType.DMA((len(places),))],
        input_output_aliases=aliases,
        compiler_params=params(),
        cost_estimate=cost(2 * rows * width * columns.shape[1], 4 * rows * width),
    )(*operands)


def halves(points, centroids, assign, share, capacity):
    rows_count = lax.axis_size("rows")
    half = rows_count // 2
    me = lax.axis_index("rows")
    total = rows_count * share
    own = lax.dynamic_slice_in_dim(centroids, me * share, share, 0)
    assign_row = assign.reshape(1, -1)

    far_rank, near_rank, far_label, near_label = ranks(assign_row, half, share)
    far = place(far_rank, far_label, points, capacity)
    far = [far[0]] + [swap(far[m], m) for m in range(1, half)]
    near = place(near_rank, near_label, points, capacity)
    near = [near[0]] + [swap(near[m], m) for m in range(1, half)]
    far_sums, far_counts = add_up(far, share, capacity)
    far_sums, late = lax.optimization_barrier((far_sums, points))
    far_sums = swap(far_sums, half)
    far_counts = swap(far_counts, half)
    columns = jnp.transpose(late)
    first = first_lowest(centroids, columns)
    near_sums, near_counts = add_up(near, share, capacity)
    pnorm = jnp.sum(jnp.square(late.astype(F32)), axis=1)
    first, pnorm, own, far_sums = lax.optimization_barrier((first, pnorm, own, far_sums))
    piece = renew(near_sums, near_counts, far_sums, far_counts, own)

    running, whole = None, None
    columns_count = rows_count // 4
    sets, corners = [], []
    for k in range(columns_count):
        one = piece if k == 0 else swap(piece, 4 * k)
        one_x, one_y = swap(one, 1), swap(one, 2)
        corner = swap(one_y, 1) if k % 2 == 0 else swap(one_x, 2)
        m = 4 * k
        sets.append([(m, 0, one), (m ^ 1, 0, one_x), (m ^ 2, 0, one_y)])
        corners.append((m ^ 3, 0, corner))
    for name, group in groups_of(columns_count):
        members = [p for k in group for p in sets[k]] if name != "last" else []
        if name != "sides":
            members += [corners[k] for k in group]
        running, whole = arrive(members, columns, running, whole, total, share)
    both = jnp.stack([jnp.min(first, axis=0), jnp.min(running, axis=0)])
    nearest = block_min((pnorm[None, :] + both) / points.shape[1])
    return nearest, whole


def groups_of(columns_count):
    early = [("set", (k,)) for k in range(columns_count - 2)]
    late = (columns_count - 2, columns_count - 1)
    return early + [("sides", late), ("last", late)]


def smallest(points, pnorm, cents):
    cnorm = jnp.sum(jnp.square(cents.astype(F32)), axis=1)
    dots = lax.dot_general(points, cents, (((1,), (1,)), ((), ())), preferred_element_type=F32)
    return jnp.min((pnorm[:, None] - 2.0 * dots + cnorm[None, :]) / points.shape[1], axis=1)


def plain(points, centroids, assign, share, capacity):
    blocksize = centroids.shape[0]
    count_pts = points.shape[0]
    pnorm = jnp.sum(jnp.square(points.astype(F32)), axis=1)
    first = smallest(points, pnorm, centroids)
    relative = assign - lax.axis_index("cent") * blocksize
    own = lax.dynamic_slice_in_dim(centroids, lax.axis_index("rows") * share, share, 0)
    rows_count = lax.axis_size("rows")
    inside = (relative >= 0) & (relative < blocksize)
    owners = jnp.where(inside, relative // share, rows_count)
    offsets = jnp.where(inside, relative - relative // share * share, 0)
    owner_hot = owners[:, None] == lax.broadcasted_iota(jnp.int32, (count_pts, rows_count), 1)
    earlier = lax.broadcasted_iota(jnp.int32, (count_pts, count_pts), 1) < lax.broadcasted_iota(
        jnp.int32, (count_pts, count_pts), 0
    )
    before = jnp.dot(earlier.astype(BF16), owner_hot.astype(BF16), preferred_element_type=F32)
    ranking = jnp.sum(jnp.where(owner_hot, before, 0.0), axis=1).astype(jnp.int32)
    slot_index = jnp.where(inside, owners * capacity + ranking, -1)
    placing = (
        lax.broadcasted_iota(jnp.int32, (rows_count * capacity, count_pts), 0)
        == slot_index[None, :]
    )
    outgoing = jnp.dot(placing.astype(BF16), points, preferred_element_type=F32).astype(BF16)
    labels = (jnp.sum(jnp.where(placing, offsets[None, :] + 1, 0), axis=1) - 1).astype(BF16)
    arrived = lax.all_to_all(outgoing, "rows", split_axis=0, concat_axis=0, tiled=True)
    arrived_labels = lax.all_to_all(labels, "rows", split_axis=0, concat_axis=0, tiled=True)
    chosen = (
        lax.broadcasted_iota(jnp.int32, (share, arrived.shape[0]), 0)
        == arrived_labels.astype(jnp.int32)[None, :]
    )
    sums = jnp.dot(chosen.astype(BF16), arrived, preferred_element_type=F32)
    counts = jnp.sum(chosen.astype(F32), axis=1)
    piece = ((sums + own.astype(F32)) / (counts[:, None] + 1.0)).astype(BF16)
    updated = lax.all_gather(piece, "rows", axis=0, tiled=True)
    second = smallest(points, pnorm, updated)
    return block_min(jnp.stack([first, second])), updated


def fits(rows_count, share, capacity, count, width, blocksize):
    return (
        rows_count >= 8
        and rows_count & (rows_count - 1) == 0
        and share % 128 == 0
        and share <= 256
        and capacity % 16 == 0
        and count % 128 == 0
        and width % 128 == 0
        and blocksize % 256 == 0
    )


def per_device(points, centroids, assign):
    rows_count = lax.axis_size("rows")
    share = centroids.shape[0] // rows_count
    groups = rows_count * lax.axis_size("cent")
    capacity = max(2, 2 * points.shape[0] // groups)
    good = fits(rows_count, share, capacity, *points.shape, centroids.shape[0])
    if not good:
        return plain(points, centroids, assign, share, capacity)
    return halves(points, centroids, assign, share, capacity)


def solution(mesh):
    return jax.shard_map(
        per_device,
        mesh=mesh,
        in_specs=(P("rows", None), P("cent", None), P("rows")),
        out_specs=(P(None, "rows"), P("cent", None)),
        check_vma=False,
    )
```

```python
import functools

import jax
import jax.numpy as jnp
from jax import lax
from jax.experimental import pallas as pl
from jax.experimental.pallas import tpu as pltpu
from jax.sharding import PartitionSpec as P


F32 = jnp.float32
BF16 = jnp.bfloat16
VMEM = pl.BlockSpec(memory_space=pltpu.VMEM)
ANY = pl.BlockSpec(memory_space=pl.ANY)
HBM = pl.BlockSpec(memory_space=pltpu.HBM)
LIMIT = 24 * 1024 * 1024
LABEL_ROWS = 8


def swap(value, mask, axis="rows"):
    size = lax.axis_size(axis)
    return lax.ppermute(value, axis, [(i, i ^ mask) for i in range(size)])


def block_min(values):
    size = lax.axis_size("cent")
    if size & (size - 1):
        return lax.pmin(values, "cent")
    mask = 1
    while mask < size:
        values = jnp.minimum(values, swap(values, mask, "cent"))
        mask *= 2
    return values


def cost(flops, moved):
    return pl.CostEstimate(flops=int(flops), bytes_accessed=int(moved), transcendentals=0)


def params():
    return pltpu.CompilerParams(vmem_limit_bytes=LIMIT)


def rank_kernel(half, share, assign_ref, far_ref, near_ref, far_label_ref, near_label_ref):
    me, cent = lax.axis_index("rows"), lax.axis_index("cent")
    count = assign_ref.shape[1]
    seg = 128
    upper = jnp.where(
        lax.broadcasted_iota(jnp.int32, (seg, seg), 0)
        < lax.broadcasted_iota(jnp.int32, (seg, seg), 1),
        1.0,
        0.0,
    ).astype(BF16)
    low = lax.rem(me, half) ^ lax.broadcasted_iota(jnp.int32, (half, count), 0)
    for side, rank_ref, label_ref in (
        (1 - me // half, far_ref, far_label_ref),
        (me // half, near_ref, near_label_ref),
    ):
        within = assign_ref[...] - (cent * 2 * half + side * half + low) * share
        hot = (within >= 0) & (within < share)
        ones = jnp.where(hot, 1.0, 0.0).astype(F32)
        total = jnp.zeros((half, 1), F32)
        before = []
        for start in range(0, count, seg):
            piece = ones[:, start : start + seg]
            before.append(jnp.dot(piece.astype(BF16), upper, preferred_element_type=F32) + total)
            total = total + jnp.sum(piece, axis=1, keepdims=True)
        rank_ref[...] = jnp.where(hot, jnp.concatenate(before, axis=1), -1.0)
        label = jnp.sum(jnp.where(hot, within + 1, 0).astype(F32), axis=0, keepdims=True)
        label_ref[...] = jnp.transpose(jnp.broadcast_to(label, (8, count))).astype(BF16)


def ranks(assign_row, half, share):
    count = assign_row.shape[1]
    rank = jax.ShapeDtypeStruct((half, count), F32)
    label = jax.ShapeDtypeStruct((count, 8), BF16)
    return pl.pallas_call(
        functools.partial(rank_kernel, half, share),
        out_shape=[rank, rank, label, label],
        in_specs=[VMEM],
        out_specs=[VMEM] * 4,
        compiler_params=params(),
        cost_estimate=cost(2e9, 64 * count),
        name="ranks",
    )(assign_row)


def place_kernel(half, capacity, rank_ref, label_ref, points_ref, *outs):
    count = points_ref.shape[0]
    slots = lax.broadcasted_iota(jnp.int32, (capacity, count), 0).astype(F32)
    placing = jnp.concatenate(
        [
            jnp.where(slots == rank_ref[m : m + 1, :], 1.0, 0.0).astype(BF16)
            for m in range(half)
        ],
        axis=0,
    )
    placed = jnp.dot(placing, points_ref[...], preferred_element_type=F32).astype(BF16)
    labels = jnp.dot(placing, label_ref[...], preferred_element_type=F32)
    labels = (jnp.transpose(labels) - 1.0).astype(BF16)
    for m in range(half):
        outs[m][:capacity, :] = placed[m * capacity : (m + 1) * capacity]
        outs[m][capacity:, :] = jnp.zeros((LABEL_ROWS, outs[m].shape[1]), BF16)
        outs[m][capacity:, :capacity] = labels[:, m * capacity : (m + 1) * capacity]


def place(rank, label, points, capacity):
    half = rank.shape[0]
    count, width = points.shape
    block = jax.ShapeDtypeStruct((capacity + LABEL_ROWS, width), BF16)
    return pl.pallas_call(
        functools.partial(place_kernel, half, capacity),
        out_shape=[block] * half,
        in_specs=[VMEM] * 3,
        out_specs=[VMEM] * half,
        compiler_params=params(),
        cost_estimate=cost(2 * half * capacity * count * width, 4 * count * width),
    )(rank, label, points)


def sum_kernel(share, capacity, *refs):
    blocks, sums_ref, counts_ref = refs[:-2], refs[-2], refs[-1]
    labels = jnp.concatenate(
        [r[capacity:, :capacity].astype(F32)[:1] for r in blocks], axis=1
    )
    chosen = jnp.where(
        lax.broadcasted_iota(jnp.int32, (share, labels.shape[1]), 0).astype(F32) == labels, 1.0, 0.0
    ).astype(F32)
    rows = jnp.concatenate([r[:capacity, :] for r in blocks], axis=0)
    sums_ref[...] = jnp.dot(chosen.astype(BF16), rows, preferred_element_type=F32)
    counts = jnp.broadcast_to(jnp.sum(chosen, axis=1, keepdims=True), (share, 8))
    counts_ref[...] = jnp.transpose(counts)


def add_up(blocks, share, capacity):
    width = blocks[0].shape[1]
    return pl.pallas_call(
        functools.partial(sum_kernel, share, capacity),
        out_shape=[jax.ShapeDtypeStruct((share, width), F32), jax.ShapeDtypeStruct((8, share), F32)],
        in_specs=[VMEM] * len(blocks),
        out_specs=[VMEM, VMEM],
        compiler_params=params(),
        cost_estimate=cost(2 * share * len(blocks) * capacity * width, 3 * share * width * 4),
    )(*blocks)


def renew_kernel(sums_ref, counts_ref, far_sums_ref, far_counts_ref, own_ref, out_ref):
    counts = jnp.transpose(counts_ref[...] + far_counts_ref[...])[:, :1]
    total = sums_ref[...] + far_sums_ref[...] + own_ref[...].astype(F32)
    out_ref[...] = (total / (counts + 1.0)).astype(BF16)


def renew(sums, counts, far_sums, far_counts, own):
    return pl.pallas_call(
        renew_kernel,
        out_shape=jax.ShapeDtypeStruct(own.shape, BF16),
        in_specs=[VMEM] * 5,
        out_specs=VMEM,
        compiler_params=params(),
        cost_estimate=cost(4 * own.size, 14 * own.size),
        name="renew",
    )(sums, counts, far_sums, far_counts, own)


def lowest(cents, columns):
    wide = cents.astype(F32)
    norms = jnp.sum(wide * wide, axis=1, keepdims=True)
    scores = norms - 2.0 * jnp.dot(cents, columns, preferred_element_type=F32)
    return jnp.min(scores.reshape(-1, 8, scores.shape[1]), axis=0)


def first_kernel(step, cents_ref, columns_ref, out_ref):
    out_ref[...] = jnp.full(out_ref.shape, jnp.inf, F32)

    @pl.loop(0, cents_ref.shape[0] // step)
    def _(i):
        start = pl.multiple_of(i * step, step)
        out_ref[...] = jnp.minimum(
            out_ref[...], lowest(cents_ref[pl.ds(start, step), :], columns_ref[...])
        )


def first_lowest(cents, columns):
    return pl.pallas_call(
        functools.partial(first_kernel, 512),
        out_shape=jax.ShapeDtypeStruct((8, columns.shape[1]), F32),
        in_specs=[VMEM, VMEM],
        out_specs=VMEM,
        compiler_params=params(),
        cost_estimate=cost(2 * cents.size * columns.shape[1], 2 * cents.size),
        name="first_lowest",
    )(cents, columns)


def arrive_kernel(share, places, fresh, *refs):
    count = len(places)
    pieces, columns_ref = refs[:count], refs[count]
    rest = refs[count + 1 :] if fresh else refs[count + 3 :]
    running_out, whole_out, sems = rest
    me = lax.axis_index("rows")
    copies = []
    for i, ((mask, row), ref) in enumerate(zip(places, pieces, strict=True)):
        start = pl.multiple_of((me ^ mask) * share + row, ref.shape[0])
        copy = pltpu.make_async_copy(
            ref, whole_out.at[pl.ds(start, ref.shape[0])], sems.at[i]
        )
        copy.start()
        copies.append(copy)
    found = lowest(jnp.concatenate([r[...] for r in pieces], axis=0), columns_ref[...])
    running_out[...] = found if fresh else jnp.minimum(refs[count + 1][...], found)
    for copy in copies:
        copy.wait()


def arrive(pieces, columns, running, whole, total, share):
    places = [(mask, row) for mask, row, _ in pieces]
    operands = [array for _, _, array in pieces]
    rows, width = sum(o.shape[0] for o in operands), operands[0].shape[1]
    fresh = running is None
    operands += [columns]
    specs = [VMEM] * len(operands)
    aliases = {}
    if not fresh:
        aliases = {len(operands) + 1: 1}
        operands += [running, whole]
        specs += [VMEM, ANY]
    return pl.pallas_call(
        functools.partial(arrive_kernel, share, places, fresh),
        out_shape=[
            jax.ShapeDtypeStruct((8, columns.shape[1]), F32),
            jax.ShapeDtypeStruct((total, width), BF16),
        ],
        in_specs=specs,
        out_specs=[VMEM, ANY],
        scratch_shapes=[pltpu.SemaphoreType.DMA((len(places),))],
        input_output_aliases=aliases,
        compiler_params=params(),
        cost_estimate=cost(2 * rows * width * columns.shape[1], 4 * rows * width),
    )(*operands)


def halves(points, centroids, assign, share, capacity):
    rows_count = lax.axis_size("rows")
    half = rows_count // 2
    me = lax.axis_index("rows")
    total = rows_count * share
    own = lax.dynamic_slice_in_dim(centroids, me * share, share, 0)
    assign_row = assign.reshape(1, -1)

    far_rank, near_rank, far_label, near_label = ranks(assign_row, half, share)
    far = place(far_rank, far_label, points, capacity)
    far = [far[0]] + [swap(far[m], m) for m in range(1, half)]
    near = place(near_rank, near_label, points, capacity)
    near = [near[0]] + [swap(near[m], m) for m in range(1, half)]
    far_sums, far_counts = add_up(far, share, capacity)
    near[1], late = lax.optimization_barrier((near[1], points))
    far_sums = swap(far_sums, half)
    far_counts = swap(far_counts, half)
    columns = jnp.transpose(late)
    first = first_lowest(centroids, columns)
    near_sums, near_counts = add_up(near, share, capacity)
    pnorm = jnp.sum(jnp.square(late.astype(F32)), axis=1)
    first, pnorm, own, far_sums = lax.optimization_barrier((first, pnorm, own, far_sums))
    piece = renew(near_sums, near_counts, far_sums, far_counts, own)

    running, whole = None, None
    columns_count = rows_count // 4
    sets, corners = [], []
    for k in range(columns_count):
        one = piece if k == 0 else swap(piece, 4 * k)
        one_y = swap(one, 2)
        one_x = swap(one, 1)
        corner = swap(one_y, 1) if k % 2 == 0 else swap(one_x, 2)
        m = 4 * k
        sets.append([(m, 0, one), (m ^ 1, 0, one_x), (m ^ 2, 0, one_y)])
        corners.append((m ^ 3, 0, corner))
    for name, group in groups_of(columns_count):
        members = [p for k in group for p in sets[k]] if name != "last" else []
        if name != "sides":
            members += [corners[k] for k in group]
        running, whole = arrive(members, columns, running, whole, total, share)
    both = jnp.stack([jnp.min(first, axis=0), jnp.min(running, axis=0)])
    nearest = block_min((pnorm[None, :] + both) / points.shape[1])
    return nearest, whole


def groups_of(columns_count):
    early = [("set", (k,)) for k in range(columns_count - 2)]
    late = (columns_count - 2, columns_count - 1)
    return early + [("sides", late), ("last", late)]


def smallest(points, pnorm, cents):
    cnorm = jnp.sum(jnp.square(cents.astype(F32)), axis=1)
    dots = lax.dot_general(points, cents, (((1,), (1,)), ((), ())), preferred_element_type=F32)
    return jnp.min((pnorm[:, None] - 2.0 * dots + cnorm[None, :]) / points.shape[1], axis=1)


def plain(points, centroids, assign, share, capacity):
    blocksize = centroids.shape[0]
    count_pts = points.shape[0]
    pnorm = jnp.sum(jnp.square(points.astype(F32)), axis=1)
    first = smallest(points, pnorm, centroids)
    relative = assign - lax.axis_index("cent") * blocksize
    own = lax.dynamic_slice_in_dim(centroids, lax.axis_index("rows") * share, share, 0)
    rows_count = lax.axis_size("rows")
    inside = (relative >= 0) & (relative < blocksize)
    owners = jnp.where(inside, relative // share, rows_count)
    offsets = jnp.where(inside, relative - relative // share * share, 0)
    owner_hot = owners[:, None] == lax.broadcasted_iota(jnp.int32, (count_pts, rows_count), 1)
    earlier = lax.broadcasted_iota(jnp.int32, (count_pts, count_pts), 1) < lax.broadcasted_iota(
        jnp.int32, (count_pts, count_pts), 0
    )
    before = jnp.dot(earlier.astype(BF16), owner_hot.astype(BF16), preferred_element_type=F32)
    ranking = jnp.sum(jnp.where(owner_hot, before, 0.0), axis=1).astype(jnp.int32)
    slot_index = jnp.where(inside, owners * capacity + ranking, -1)
    placing = (
        lax.broadcasted_iota(jnp.int32, (rows_count * capacity, count_pts), 0)
        == slot_index[None, :]
    )
    outgoing = jnp.dot(placing.astype(BF16), points, preferred_element_type=F32).astype(BF16)
    labels = (jnp.sum(jnp.where(placing, offsets[None, :] + 1, 0), axis=1) - 1).astype(BF16)
    arrived = lax.all_to_all(outgoing, "rows", split_axis=0, concat_axis=0, tiled=True)
    arrived_labels = lax.all_to_all(labels, "rows", split_axis=0, concat_axis=0, tiled=True)
    chosen = (
        lax.broadcasted_iota(jnp.int32, (share, arrived.shape[0]), 0)
        == arrived_labels.astype(jnp.int32)[None, :]
    )
    sums = jnp.dot(chosen.astype(BF16), arrived, preferred_element_type=F32)
    counts = jnp.sum(chosen.astype(F32), axis=1)
    piece = ((sums + own.astype(F32)) / (counts[:, None] + 1.0)).astype(BF16)
    updated = lax.all_gather(piece, "rows", axis=0, tiled=True)
    second = smallest(points, pnorm, updated)
    return block_min(jnp.stack([first, second])), updated


def fits(rows_count, share, capacity, count, width, blocksize):
    return (
        rows_count >= 8
        and rows_count & (rows_count - 1) == 0
        and share % 128 == 0
        and share <= 256
        and capacity % 16 == 0
        and count % 128 == 0
        and width % 128 == 0
        and blocksize % 256 == 0
    )


def per_device(points, centroids, assign):
    rows_count = lax.axis_size("rows")
    share = centroids.shape[0] // rows_count
    groups = rows_count * lax.axis_size("cent")
    capacity = max(2, 2 * points.shape[0] // groups)
    good = fits(rows_count, share, capacity, *points.shape, centroids.shape[0])
    if not good:
        return plain(points, centroids, assign, share, capacity)
    return halves(points, centroids, assign, share, capacity)


def solution(mesh):
    return jax.shard_map(
        per_device,
        mesh=mesh,
        in_specs=(P("rows", None), P("cent", None), P("rows")),
        out_specs=(P(None, "rows"), P("cent", None)),
        check_vma=False,
    )
```

```python
import functools

import jax
import jax.numpy as jnp
from jax import lax
from jax.experimental import pallas as pl
from jax.experimental.pallas import tpu as pltpu
from jax.sharding import PartitionSpec as P


F32 = jnp.float32
BF16 = jnp.bfloat16
VMEM = pl.BlockSpec(memory_space=pltpu.VMEM)
ANY = pl.BlockSpec(memory_space=pl.ANY)
HBM = pl.BlockSpec(memory_space=pltpu.HBM)
LIMIT = 24 * 1024 * 1024
LABEL_ROWS = 8


def swap(value, mask, axis="rows"):
    size = lax.axis_size(axis)
    return lax.ppermute(value, axis, [(i, i ^ mask) for i in range(size)])


def block_min(values):
    size = lax.axis_size("cent")
    if size & (size - 1):
        return lax.pmin(values, "cent")
    mask = 1
    while mask < size:
        values = jnp.minimum(values, swap(values, mask, "cent"))
        mask *= 2
    return values


def cost(flops, moved):
    return pl.CostEstimate(flops=int(flops), bytes_accessed=int(moved), transcendentals=0)


def params():
    return pltpu.CompilerParams(vmem_limit_bytes=LIMIT)


def rank_kernel(half, share, assign_ref, far_ref, near_ref, far_label_ref, near_label_ref):
    me, cent = lax.axis_index("rows"), lax.axis_index("cent")
    count = assign_ref.shape[1]
    seg = 128
    upper = jnp.where(
        lax.broadcasted_iota(jnp.int32, (seg, seg), 0)
        < lax.broadcasted_iota(jnp.int32, (seg, seg), 1),
        1.0,
        0.0,
    ).astype(BF16)
    low = lax.rem(me, half) ^ lax.broadcasted_iota(jnp.int32, (half, count), 0)
    for side, rank_ref, label_ref in (
        (1 - me // half, far_ref, far_label_ref),
        (me // half, near_ref, near_label_ref),
    ):
        within = assign_ref[...] - (cent * 2 * half + side * half + low) * share
        hot = (within >= 0) & (within < share)
        ones = jnp.where(hot, 1.0, 0.0).astype(F32)
        total = jnp.zeros((half, 1), F32)
        before = []
        for start in range(0, count, seg):
            piece = ones[:, start : start + seg]
            before.append(jnp.dot(piece.astype(BF16), upper, preferred_element_type=F32) + total)
            total = total + jnp.sum(piece, axis=1, keepdims=True)
        rank_ref[...] = jnp.where(hot, jnp.concatenate(before, axis=1), -1.0)
        label = jnp.sum(jnp.where(hot, within + 1, 0).astype(F32), axis=0, keepdims=True)
        label_ref[...] = jnp.transpose(jnp.broadcast_to(label, (8, count))).astype(BF16)


def ranks(assign_row, half, share):
    count = assign_row.shape[1]
    rank = jax.ShapeDtypeStruct((half, count), F32)
    label = jax.ShapeDtypeStruct((count, 8), BF16)
    return pl.pallas_call(
        functools.partial(rank_kernel, half, share),
        out_shape=[rank, rank, label, label],
        in_specs=[VMEM],
        out_specs=[VMEM] * 4,
        compiler_params=params(),
        cost_estimate=cost(2e9, 64 * count),
        name="ranks",
    )(assign_row)


def place_kernel(half, capacity, rank_ref, label_ref, points_ref, *outs):
    count = points_ref.shape[0]
    slots = lax.broadcasted_iota(jnp.int32, (capacity, count), 0).astype(F32)
    placing = jnp.concatenate(
        [
            jnp.where(slots == rank_ref[m : m + 1, :], 1.0, 0.0).astype(BF16)
            for m in range(half)
        ],
        axis=0,
    )
    placed = jnp.dot(placing, points_ref[...], preferred_element_type=F32).astype(BF16)
    labels = jnp.dot(placing, label_ref[...], preferred_element_type=F32)
    labels = (jnp.transpose(labels) - 1.0).astype(BF16)
    for m in range(half):
        outs[m][:capacity, :] = placed[m * capacity : (m + 1) * capacity]
        outs[m][capacity:, :] = jnp.zeros((LABEL_ROWS, outs[m].shape[1]), BF16)
        outs[m][capacity:, :capacity] = labels[:, m * capacity : (m + 1) * capacity]


def place(rank, label, points, capacity):
    half = rank.shape[0]
    count, width = points.shape
    block = jax.ShapeDtypeStruct((capacity + LABEL_ROWS, width), BF16)
    return pl.pallas_call(
        functools.partial(place_kernel, half, capacity),
        out_shape=[block] * half,
        in_specs=[VMEM] * 3,
        out_specs=[VMEM] * half,
        compiler_params=params(),
        cost_estimate=cost(2 * half * capacity * count * width, 4 * count * width),
    )(rank, label, points)


def sum_kernel(share, capacity, *refs):
    blocks, sums_ref, counts_ref = refs[:-2], refs[-2], refs[-1]
    labels = jnp.concatenate(
        [r[capacity:, :capacity].astype(F32)[:1] for r in blocks], axis=1
    )
    chosen = jnp.where(
        lax.broadcasted_iota(jnp.int32, (share, labels.shape[1]), 0).astype(F32) == labels, 1.0, 0.0
    ).astype(F32)
    rows = jnp.concatenate([r[:capacity, :] for r in blocks], axis=0)
    sums_ref[...] = jnp.dot(chosen.astype(BF16), rows, preferred_element_type=F32)
    counts = jnp.broadcast_to(jnp.sum(chosen, axis=1, keepdims=True), (share, 8))
    counts_ref[...] = jnp.transpose(counts)


def add_up(blocks, share, capacity):
    width = blocks[0].shape[1]
    return pl.pallas_call(
        functools.partial(sum_kernel, share, capacity),
        out_shape=[jax.ShapeDtypeStruct((share, width), F32), jax.ShapeDtypeStruct((8, share), F32)],
        in_specs=[VMEM] * len(blocks),
        out_specs=[VMEM, VMEM],
        compiler_params=params(),
        cost_estimate=cost(2 * share * len(blocks) * capacity * width, 3 * share * width * 4),
    )(*blocks)


def renew_kernel(sums_ref, counts_ref, far_sums_ref, far_counts_ref, own_ref, out_ref):
    counts = jnp.transpose(counts_ref[...] + far_counts_ref[...])[:, :1]
    total = sums_ref[...] + far_sums_ref[...] + own_ref[...].astype(F32)
    out_ref[...] = (total / (counts + 1.0)).astype(BF16)


def renew(sums, counts, far_sums, far_counts, own):
    return pl.pallas_call(
        renew_kernel,
        out_shape=jax.ShapeDtypeStruct(own.shape, BF16),
        in_specs=[VMEM] * 5,
        out_specs=VMEM,
        compiler_params=params(),
        cost_estimate=cost(4 * own.size, 14 * own.size),
        name="renew",
    )(sums, counts, far_sums, far_counts, own)


def lowest(cents, columns):
    wide = cents.astype(F32)
    norms = jnp.sum(wide * wide, axis=1, keepdims=True)
    scores = norms - 2.0 * jnp.dot(cents, columns, preferred_element_type=F32)
    return jnp.min(scores.reshape(-1, 8, scores.shape[1]), axis=0)


def first_kernel(step, cents_ref, columns_ref, out_ref):
    out_ref[...] = jnp.full(out_ref.shape, jnp.inf, F32)

    @pl.loop(0, cents_ref.shape[0] // step)
    def _(i):
        start = pl.multiple_of(i * step, step)
        out_ref[...] = jnp.minimum(
            out_ref[...], lowest(cents_ref[pl.ds(start, step), :], columns_ref[...])
        )


def first_lowest(cents, columns):
    return pl.pallas_call(
        functools.partial(first_kernel, 512),
        out_shape=jax.ShapeDtypeStruct((8, columns.shape[1]), F32),
        in_specs=[VMEM, VMEM],
        out_specs=VMEM,
        compiler_params=params(),
        cost_estimate=cost(2 * cents.size * columns.shape[1], 2 * cents.size),
        name="first_lowest",
    )(cents, columns)


def arrive_kernel(share, places, fresh, *refs):
    count = len(places)
    pieces, columns_ref = refs[:count], refs[count]
    rest = refs[count + 1 :] if fresh else refs[count + 3 :]
    running_out, whole_out, sems = rest
    me = lax.axis_index("rows")
    copies = []
    for i, ((mask, row), ref) in enumerate(zip(places, pieces, strict=True)):
        start = pl.multiple_of((me ^ mask) * share + row, ref.shape[0])
        copy = pltpu.make_async_copy(
            ref, whole_out.at[pl.ds(start, ref.shape[0])], sems.at[i]
        )
        copy.start()
        copies.append(copy)
    found = lowest(jnp.concatenate([r[...] for r in pieces], axis=0), columns_ref[...])
    running_out[...] = found if fresh else jnp.minimum(refs[count + 1][...], found)
    for copy in copies:
        copy.wait()


def low_kernel(*refs):
    pieces, (columns_ref, running_ref, out_ref) = refs[:-3], refs[-3:]
    found = lowest(jnp.concatenate([r[...] for r in pieces], axis=0), columns_ref[...])
    out_ref[...] = jnp.minimum(running_ref[...], found)


def write_kernel(share, places, *refs):
    count = len(places)
    pieces, (whole_out, held, in_sems, out_sems) = refs[:count], refs[count + 1 :]
    me = lax.axis_index("rows")
    moves, at = [], 0
    for i, ((mask, row), ref) in enumerate(zip(places, pieces, strict=True)):
        rows = ref.shape[0]
        slot = held.at[pl.ds(at, rows)]
        start = pl.multiple_of((me ^ mask) * share + row, rows)
        inward = pltpu.make_async_copy(ref, slot, in_sems.at[i])
        outward = pltpu.make_async_copy(slot, whole_out.at[pl.ds(start, rows)], out_sems.at[i])
        inward.start()
        moves.append((inward, outward))
        at += rows
    for inward, outward in moves:
        inward.wait()
        outward.start()
    for _, outward in moves:
        outward.wait()


def write(pieces, whole, share):
    places = [(mask, row) for mask, row, _ in pieces]
    operands = [array for _, _, array in pieces]
    rows, width = sum(o.shape[0] for o in operands), operands[0].shape[1]
    return pl.pallas_call(
        functools.partial(write_kernel, share, places),
        out_shape=jax.ShapeDtypeStruct(whole.shape, whole.dtype),
        in_specs=[ANY] * (len(operands) + 1),
        out_specs=ANY,
        scratch_shapes=[
            pltpu.VMEM((rows, width), BF16),
            pltpu.SemaphoreType.DMA((len(places),)),
            pltpu.SemaphoreType.DMA((len(places),)),
        ],
        input_output_aliases={len(operands): 0},
        compiler_params=params(),
        cost_estimate=cost(rows * width, 4 * rows * width),
        name="write_last",
    )(*operands, whole)


def arrive(pieces, columns, running, whole, total, share, writes=True):
    places = [(mask, row) for mask, row, _ in pieces]
    operands = [array for _, _, array in pieces]
    rows, width = sum(o.shape[0] for o in operands), operands[0].shape[1]
    fresh = running is None
    if not writes:
        return pl.pallas_call(
            low_kernel,
            out_shape=jax.ShapeDtypeStruct((8, columns.shape[1]), F32),
            in_specs=[VMEM] * (len(operands) + 2),
            out_specs=VMEM,
            compiler_params=params(),
            cost_estimate=cost(2 * rows * width * columns.shape[1], 2 * rows * width),
        )(*operands, columns, running), whole
    operands += [columns]
    specs = [VMEM] * len(operands)
    aliases = {}
    if not fresh:
        aliases = {len(operands) + 1: 1}
        operands += [running, whole]
        specs += [VMEM, ANY]
    return pl.pallas_call(
        functools.partial(arrive_kernel, share, places, fresh),
        out_shape=[
            jax.ShapeDtypeStruct((8, columns.shape[1]), F32),
            jax.ShapeDtypeStruct((total, width), BF16),
        ],
        in_specs=specs,
        out_specs=[VMEM, ANY],
        scratch_shapes=[pltpu.SemaphoreType.DMA((len(places),))],
        input_output_aliases=aliases,
        compiler_params=params(),
        cost_estimate=cost(2 * rows * width * columns.shape[1], 4 * rows * width),
    )(*operands)


def halves(points, centroids, assign, share, capacity):
    rows_count = lax.axis_size("rows")
    half = rows_count // 2
    me = lax.axis_index("rows")
    total = rows_count * share
    own = lax.dynamic_slice_in_dim(centroids, me * share, share, 0)
    assign_row = assign.reshape(1, -1)

    far_rank, near_rank, far_label, near_label = ranks(assign_row, half, share)
    far = place(far_rank, far_label, points, capacity)
    far = [far[0]] + [swap(far[m], m) for m in range(1, half)]
    near = place(near_rank, near_label, points, capacity)
    near = [near[0]] + [swap(near[m], m) for m in range(1, half)]
    far_sums, far_counts = add_up(far, share, capacity)
    near[1], late = lax.optimization_barrier((near[1], points))
    far_sums = swap(far_sums, half)
    far_counts = swap(far_counts, half)
    columns = jnp.transpose(late)
    first = first_lowest(centroids, columns)
    near_sums, near_counts = add_up(near, share, capacity)
    pnorm = jnp.sum(jnp.square(late.astype(F32)), axis=1)
    first, pnorm, own, far_sums = lax.optimization_barrier((first, pnorm, own, far_sums))
    piece = renew(near_sums, near_counts, far_sums, far_counts, own)

    running, whole = None, None
    columns_count = rows_count // 4
    sets, corners = [], []
    for k in range(columns_count):
        one = piece if k == 0 else swap(piece, 4 * k)
        one_y = swap(one, 2)
        one_x = swap(one, 1)
        corner = swap(one_y, 1) if k % 2 == 0 else swap(one_x, 2)
        m = 4 * k
        sets.append([(m, 0, one), (m ^ 1, 0, one_x), (m ^ 2, 0, one_y)])
        corners.append((m ^ 3, 0, corner))
    for name, group in groups_of(columns_count):
        members = [p for k in group for p in sets[k]] if name == "set" else []
        if name == "set":
            members += [corners[k] for k in group]
            if group[0] == columns_count - 3:
                members += [sets[k][0] for k in range(columns_count - 2, columns_count)]
        elif name == "sides":
            members = [p for k in group for p in sets[k][1:]]
        else:
            members = [corners[k] for k in group]
        running, whole = arrive(members, columns, running, whole, total, share, name != "last")
    whole = write([corners[k] for k in group], whole, share)
    both = jnp.stack([jnp.min(first, axis=0), jnp.min(running, axis=0)])
    nearest = block_min((pnorm[None, :] + both) / points.shape[1])
    return nearest, whole


def groups_of(columns_count):
    early = [("set", (k,)) for k in range(columns_count - 2)]
    late = (columns_count - 2, columns_count - 1)
    return early + [("sides", late), ("last", late)]


def smallest(points, pnorm, cents):
    cnorm = jnp.sum(jnp.square(cents.astype(F32)), axis=1)
    dots = lax.dot_general(points, cents, (((1,), (1,)), ((), ())), preferred_element_type=F32)
    return jnp.min((pnorm[:, None] - 2.0 * dots + cnorm[None, :]) / points.shape[1], axis=1)


def plain(points, centroids, assign, share, capacity):
    blocksize = centroids.shape[0]
    count_pts = points.shape[0]
    pnorm = jnp.sum(jnp.square(points.astype(F32)), axis=1)
    first = smallest(points, pnorm, centroids)
    relative = assign - lax.axis_index("cent") * blocksize
    own = lax.dynamic_slice_in_dim(centroids, lax.axis_index("rows") * share, share, 0)
    rows_count = lax.axis_size("rows")
    inside = (relative >= 0) & (relative < blocksize)
    owners = jnp.where(inside, relative // share, rows_count)
    offsets = jnp.where(inside, relative - relative // share * share, 0)
    owner_hot = owners[:, None] == lax.broadcasted_iota(jnp.int32, (count_pts, rows_count), 1)
    earlier = lax.broadcasted_iota(jnp.int32, (count_pts, count_pts), 1) < lax.broadcasted_iota(
        jnp.int32, (count_pts, count_pts), 0
    )
    before = jnp.dot(earlier.astype(BF16), owner_hot.astype(BF16), preferred_element_type=F32)
    ranking = jnp.sum(jnp.where(owner_hot, before, 0.0), axis=1).astype(jnp.int32)
    slot_index = jnp.where(inside, owners * capacity + ranking, -1)
    placing = (
        lax.broadcasted_iota(jnp.int32, (rows_count * capacity, count_pts), 0)
        == slot_index[None, :]
    )
    outgoing = jnp.dot(placing.astype(BF16), points, preferred_element_type=F32).astype(BF16)
    labels = (jnp.sum(jnp.where(placing, offsets[None, :] + 1, 0), axis=1) - 1).astype(BF16)
    arrived = lax.all_to_all(outgoing, "rows", split_axis=0, concat_axis=0, tiled=True)
    arrived_labels = lax.all_to_all(labels, "rows", split_axis=0, concat_axis=0, tiled=True)
    chosen = (
        lax.broadcasted_iota(jnp.int32, (share, arrived.shape[0]), 0)
        == arrived_labels.astype(jnp.int32)[None, :]
    )
    sums = jnp.dot(chosen.astype(BF16), arrived, preferred_element_type=F32)
    counts = jnp.sum(chosen.astype(F32), axis=1)
    piece = ((sums + own.astype(F32)) / (counts[:, None] + 1.0)).astype(BF16)
    updated = lax.all_gather(piece, "rows", axis=0, tiled=True)
    second = smallest(points, pnorm, updated)
    return block_min(jnp.stack([first, second])), updated


def fits(rows_count, share, capacity, count, width, blocksize):
    return (
        rows_count >= 8
        and rows_count & (rows_count - 1) == 0
        and share % 128 == 0
        and share <= 256
        and capacity % 16 == 0
        and count % 128 == 0
        and width % 128 == 0
        and blocksize % 256 == 0
    )


def per_device(points, centroids, assign):
    rows_count = lax.axis_size("rows")
    share = centroids.shape[0] // rows_count
    groups = rows_count * lax.axis_size("cent")
    capacity = max(2, 2 * points.shape[0] // groups)
    good = fits(rows_count, share, capacity, *points.shape, centroids.shape[0])
    if not good:
        return plain(points, centroids, assign, share, capacity)
    return halves(points, centroids, assign, share, capacity)


def solution(mesh):
    return jax.shard_map(
        per_device,
        mesh=mesh,
        in_specs=(P("rows", None), P("cent", None), P("rows")),
        out_specs=(P(None, "rows"), P("cent", None)),
        check_vma=False,
    )
```

```python
import functools

import jax
import jax.numpy as jnp
from jax import lax
from jax.experimental import pallas as pl
from jax.experimental.pallas import tpu as pltpu
from jax.sharding import PartitionSpec as P


F32 = jnp.float32
BF16 = jnp.bfloat16
VMEM = pl.BlockSpec(memory_space=pltpu.VMEM)
ANY = pl.BlockSpec(memory_space=pl.ANY)
HBM = pl.BlockSpec(memory_space=pltpu.HBM)
LIMIT = 24 * 1024 * 1024
WIDE = 58 * 1024 * 1024
LABEL_ROWS = 8


def swap(value, mask, axis="rows"):
    size = lax.axis_size(axis)
    return lax.ppermute(value, axis, [(i, i ^ mask) for i in range(size)])


def block_min(values):
    size = lax.axis_size("cent")
    if size & (size - 1):
        return lax.pmin(values, "cent")
    mask = 1
    while mask < size:
        values = jnp.minimum(values, swap(values, mask, "cent"))
        mask *= 2
    return values


def cost(flops, moved):
    return pl.CostEstimate(flops=int(flops), bytes_accessed=int(moved), transcendentals=0)


def params():
    return pltpu.CompilerParams(vmem_limit_bytes=LIMIT)


def rank_kernel(half, share, assign_ref, far_ref, near_ref, far_label_ref, near_label_ref):
    me, cent = lax.axis_index("rows"), lax.axis_index("cent")
    count = assign_ref.shape[1]
    seg = 128
    upper = jnp.where(
        lax.broadcasted_iota(jnp.int32, (seg, seg), 0)
        < lax.broadcasted_iota(jnp.int32, (seg, seg), 1),
        1.0,
        0.0,
    ).astype(BF16)
    low = lax.rem(me, half) ^ lax.broadcasted_iota(jnp.int32, (half, count), 0)
    for side, rank_ref, label_ref in (
        (1 - me // half, far_ref, far_label_ref),
        (me // half, near_ref, near_label_ref),
    ):
        within = assign_ref[...] - (cent * 2 * half + side * half + low) * share
        hot = (within >= 0) & (within < share)
        ones = jnp.where(hot, 1.0, 0.0).astype(F32)
        total = jnp.zeros((half, 1), F32)
        before = []
        for start in range(0, count, seg):
            piece = ones[:, start : start + seg]
            before.append(jnp.dot(piece.astype(BF16), upper, preferred_element_type=F32) + total)
            total = total + jnp.sum(piece, axis=1, keepdims=True)
        rank_ref[...] = jnp.where(hot, jnp.concatenate(before, axis=1), -1.0)
        label = jnp.sum(jnp.where(hot, within + 1, 0).astype(F32), axis=0, keepdims=True)
        label_ref[...] = jnp.transpose(jnp.broadcast_to(label, (8, count))).astype(BF16)


def ranks(assign_row, half, share):
    count = assign_row.shape[1]
    rank = jax.ShapeDtypeStruct((half, count), F32)
    label = jax.ShapeDtypeStruct((count, 8), BF16)
    return pl.pallas_call(
        functools.partial(rank_kernel, half, share),
        out_shape=[rank, rank, label, label],
        in_specs=[VMEM],
        out_specs=[VMEM] * 4,
        compiler_params=params(),
        cost_estimate=cost(2e9, 64 * count),
        name="ranks",
    )(assign_row)


def place_kernel(masks, capacity, rank_ref, label_ref, points_ref, *outs):
    count = points_ref.shape[0]
    slots = lax.broadcasted_iota(jnp.int32, (capacity, count), 0).astype(F32)
    placing = jnp.concatenate(
        [
            jnp.where(slots == rank_ref[m : m + 1, :], 1.0, 0.0).astype(BF16)
            for m in masks
        ],
        axis=0,
    )
    placed = jnp.dot(placing, points_ref[...], preferred_element_type=F32).astype(BF16)
    labels = jnp.dot(placing, label_ref[...], preferred_element_type=F32)
    labels = (jnp.transpose(labels) - 1.0).astype(BF16)
    for m in range(len(masks)):
        outs[m][:capacity, :] = placed[m * capacity : (m + 1) * capacity]
        outs[m][capacity:, :] = jnp.zeros((LABEL_ROWS, outs[m].shape[1]), BF16)
        outs[m][capacity:, :capacity] = labels[:, m * capacity : (m + 1) * capacity]


def place(rank, label, points, capacity, masks):
    half = len(masks)
    count, width = points.shape
    block = jax.ShapeDtypeStruct((capacity + LABEL_ROWS, width), BF16)
    blocks = pl.pallas_call(
        functools.partial(place_kernel, masks, capacity),
        out_shape=[block] * half,
        in_specs=[VMEM] * 3,
        out_specs=[VMEM] * half,
        compiler_params=params(),
        cost_estimate=cost(2 * half * capacity * count * width, 4 * count * width),
    )(rank, label, points)
    return dict(zip(masks, blocks, strict=True))


def sum_kernel(share, capacity, *refs):
    blocks, sums_ref, counts_ref = refs[:-2], refs[-2], refs[-1]
    labels = jnp.concatenate(
        [r[capacity:, :capacity].astype(F32)[:1] for r in blocks], axis=1
    )
    chosen = jnp.where(
        lax.broadcasted_iota(jnp.int32, (share, labels.shape[1]), 0).astype(F32) == labels, 1.0, 0.0
    ).astype(F32)
    rows = jnp.concatenate([r[:capacity, :] for r in blocks], axis=0)
    sums_ref[...] = jnp.dot(chosen.astype(BF16), rows, preferred_element_type=F32)
    counts = jnp.broadcast_to(jnp.sum(chosen, axis=1, keepdims=True), (share, 8))
    counts_ref[...] = jnp.transpose(counts)


def add_up(blocks, share, capacity):
    width = blocks[0].shape[1]
    return pl.pallas_call(
        functools.partial(sum_kernel, share, capacity),
        out_shape=[jax.ShapeDtypeStruct((share, width), F32), jax.ShapeDtypeStruct((8, share), F32)],
        in_specs=[VMEM] * len(blocks),
        out_specs=[VMEM, VMEM],
        compiler_params=params(),
        cost_estimate=cost(2 * share * len(blocks) * capacity * width, 3 * share * width * 4),
    )(*blocks)


def renew_kernel(sums_ref, counts_ref, far_sums_ref, far_counts_ref, own_ref, out_ref):
    counts = jnp.transpose(counts_ref[...] + far_counts_ref[...])[:, :1]
    total = sums_ref[...] + far_sums_ref[...] + own_ref[...].astype(F32)
    out_ref[...] = (total / (counts + 1.0)).astype(BF16)


def renew(sums, counts, far_sums, far_counts, own):
    return pl.pallas_call(
        renew_kernel,
        out_shape=jax.ShapeDtypeStruct(own.shape, BF16),
        in_specs=[VMEM] * 5,
        out_specs=VMEM,
        compiler_params=params(),
        cost_estimate=cost(4 * own.size, 14 * own.size),
        name="renew",
    )(sums, counts, far_sums, far_counts, own)


def lowest(cents, columns):
    wide = cents.astype(F32)
    norms = jnp.sum(wide * wide, axis=1, keepdims=True)
    scores = norms - 2.0 * jnp.dot(cents, columns, preferred_element_type=F32)
    return jnp.min(scores.reshape(-1, 8, scores.shape[1]), axis=0)


def first_kernel(cents_ref, columns_ref, out_ref):
    found = lowest(cents_ref[...], columns_ref[...])

    @pl.when(pl.program_id(0) == 0)
    def _():
        out_ref[...] = found

    @pl.when(pl.program_id(0) > 0)
    def _():
        out_ref[...] = jnp.minimum(out_ref[...], found)


def first_lowest(cents, columns):
    count, width = cents.shape
    step = 512 if count % 512 == 0 else 256
    out = jax.ShapeDtypeStruct((8, columns.shape[1]), F32)
    return pl.pallas_call(
        first_kernel,
        grid=(count // step,),
        out_shape=out,
        in_specs=[pl.BlockSpec((step, width), lambda i: (i, 0)), VMEM],
        out_specs=pl.BlockSpec(out.shape, lambda i: (0, 0)),
        compiler_params=pltpu.CompilerParams(vmem_limit_bytes=WIDE),
        cost_estimate=cost(2 * cents.size * columns.shape[1], 2 * cents.size),
        name="first_lowest",
    )(cents, columns)


def arrive_kernel(share, places, fresh, *refs):
    count = len(places)
    pieces, columns_ref = refs[:count], refs[count]
    rest = refs[count + 1 :] if fresh else refs[count + 3 :]
    running_out, whole_out, sems = rest
    me = lax.axis_index("rows")
    copies = []
    for i, ((mask, row), ref) in enumerate(zip(places, pieces, strict=True)):
        start = pl.multiple_of((me ^ mask) * share + row, ref.shape[0])
        copy = pltpu.make_async_copy(
            ref, whole_out.at[pl.ds(start, ref.shape[0])], sems.at[i]
        )
        copy.start()
        copies.append(copy)
    found = lowest(jnp.concatenate([r[...] for r in pieces], axis=0), columns_ref[...])
    running_out[...] = found if fresh else jnp.minimum(refs[count + 1][...], found)
    for copy in copies:
        copy.wait()


def low_kernel(*refs):
    pieces, (columns_ref, running_ref, out_ref) = refs[:-3], refs[-3:]
    found = lowest(jnp.concatenate([r[...] for r in pieces], axis=0), columns_ref[...])
    out_ref[...] = jnp.minimum(running_ref[...], found)


def write_kernel(share, places, *refs):
    count = len(places)
    pieces, (whole_out, held, in_sems, out_sems) = refs[:count], refs[count + 1 :]
    me = lax.axis_index("rows")
    moves, at = [], 0
    for i, ((mask, row), ref) in enumerate(zip(places, pieces, strict=True)):
        rows = ref.shape[0]
        slot = held.at[pl.ds(at, rows)]
        start = pl.multiple_of((me ^ mask) * share + row, rows)
        inward = pltpu.make_async_copy(ref, slot, in_sems.at[i])
        outward = pltpu.make_async_copy(slot, whole_out.at[pl.ds(start, rows)], out_sems.at[i])
        inward.start()
        moves.append((inward, outward))
        at += rows
    for inward, outward in moves:
        inward.wait()
        outward.start()
    for _, outward in moves:
        outward.wait()


def write(pieces, whole, share):
    places = [(mask, row) for mask, row, _ in pieces]
    operands = [array for _, _, array in pieces]
    rows, width = sum(o.shape[0] for o in operands), operands[0].shape[1]
    return pl.pallas_call(
        functools.partial(write_kernel, share, places),
        out_shape=jax.ShapeDtypeStruct(whole.shape, whole.dtype),
        in_specs=[ANY] * (len(operands) + 1),
        out_specs=ANY,
        scratch_shapes=[
            pltpu.VMEM((rows, width), BF16),
            pltpu.SemaphoreType.DMA((len(places),)),
            pltpu.SemaphoreType.DMA((len(places),)),
        ],
        input_output_aliases={len(operands): 0},
        compiler_params=params(),
        cost_estimate=cost(rows * width, 4 * rows * width),
        name="write_last",
    )(*operands, whole)


def arrive(pieces, columns, running, whole, total, share, writes=True):
    places = [(mask, row) for mask, row, _ in pieces]
    operands = [array for _, _, array in pieces]
    rows, width = sum(o.shape[0] for o in operands), operands[0].shape[1]
    fresh = running is None
    if not writes:
        return pl.pallas_call(
            low_kernel,
            out_shape=jax.ShapeDtypeStruct((8, columns.shape[1]), F32),
            in_specs=[VMEM] * (len(operands) + 2),
            out_specs=VMEM,
            compiler_params=params(),
            cost_estimate=cost(2 * rows * width * columns.shape[1], 2 * rows * width),
        )(*operands, columns, running), whole
    operands += [columns]
    specs = [VMEM] * len(operands)
    aliases = {}
    if not fresh:
        aliases = {len(operands) + 1: 1}
        operands += [running, whole]
        specs += [VMEM, ANY]
    return pl.pallas_call(
        functools.partial(arrive_kernel, share, places, fresh),
        out_shape=[
            jax.ShapeDtypeStruct((8, columns.shape[1]), F32),
            jax.ShapeDtypeStruct((total, width), BF16),
        ],
        in_specs=specs,
        out_specs=[VMEM, ANY],
        scratch_shapes=[pltpu.SemaphoreType.DMA((len(places),))],
        input_output_aliases=aliases,
        compiler_params=params(),
        cost_estimate=cost(2 * rows * width * columns.shape[1], 4 * rows * width),
    )(*operands)


def halves(points, centroids, assign, share, capacity):
    rows_count = lax.axis_size("rows")
    half = rows_count // 2
    me = lax.axis_index("rows")
    total = rows_count * share
    own = lax.dynamic_slice_in_dim(centroids, me * share, share, 0)
    assign_row = assign.reshape(1, -1)

    far_rank, near_rank, far_label, near_label = ranks(assign_row, half, share)
    powers = [m for m in range(half) if m and m & (m - 1) == 0]
    others = [m for m in range(half) if m not in powers]
    far = place(far_rank, far_label, points, capacity, powers)
    far |= place(far_rank, far_label, points, capacity, others)
    far = [far[0]] + [swap(far[m], m) for m in range(1, half)]
    near = place(near_rank, near_label, points, capacity, range(half))
    near = [near[0]] + [swap(near[m], m) for m in range(1, half)]
    far_sums, far_counts = add_up(far, share, capacity)
    near[1], late = lax.optimization_barrier((near[1], points))
    far_sums = swap(far_sums, half)
    far_counts = swap(far_counts, half)
    columns = jnp.transpose(late)
    first = first_lowest(centroids, columns)
    near_sums, near_counts = add_up(near, share, capacity)
    pnorm = jnp.sum(jnp.square(late.astype(F32)), axis=1)
    first, pnorm, own, far_sums = lax.optimization_barrier((first, pnorm, own, far_sums))
    piece = renew(near_sums, near_counts, far_sums, far_counts, own)

    running, whole = None, None
    columns_count = rows_count // 4
    sets, corners = [], []
    for k in range(columns_count):
        one = piece if k == 0 else swap(piece, 4 * k)
        one_y = swap(one, 2)
        one_x = swap(one, 1)
        corner = swap(one_y, 1) if k % 2 == 0 else swap(one_x, 2)
        m = 4 * k
        sets.append([(m, 0, one), (m ^ 1, 0, one_x), (m ^ 2, 0, one_y)])
        corners.append((m ^ 3, 0, corner))
    for name, group in groups_of(columns_count):
        members = [p for k in group for p in sets[k]] if name == "set" else []
        if name == "set":
            members += [corners[k] for k in group]
            if group[0] == columns_count - 3:
                members += [sets[k][0] for k in range(columns_count - 2, columns_count)]
        elif name == "sides":
            members = [p for k in group for p in sets[k][1:]]
        else:
            members = [corners[k] for k in group]
        running, whole = arrive(members, columns, running, whole, total, share, name != "last")
    whole = write([corners[k] for k in group], whole, share)
    both = jnp.stack([jnp.min(first, axis=0), jnp.min(running, axis=0)])
    nearest = block_min((pnorm[None, :] + both) / points.shape[1])
    return nearest, whole


def groups_of(columns_count):
    early = [("set", (k,)) for k in range(columns_count - 2)]
    late = (columns_count - 2, columns_count - 1)
    return early + [("sides", late), ("last", late)]


def smallest(points, pnorm, cents):
    cnorm = jnp.sum(jnp.square(cents.astype(F32)), axis=1)
    dots = lax.dot_general(points, cents, (((1,), (1,)), ((), ())), preferred_element_type=F32)
    return jnp.min((pnorm[:, None] - 2.0 * dots + cnorm[None, :]) / points.shape[1], axis=1)


def plain(points, centroids, assign, share, capacity):
    blocksize = centroids.shape[0]
    count_pts = points.shape[0]
    pnorm = jnp.sum(jnp.square(points.astype(F32)), axis=1)
    first = smallest(points, pnorm, centroids)
    relative = assign - lax.axis_index("cent") * blocksize
    own = lax.dynamic_slice_in_dim(centroids, lax.axis_index("rows") * share, share, 0)
    rows_count = lax.axis_size("rows")
    inside = (relative >= 0) & (relative < blocksize)
    owners = jnp.where(inside, relative // share, rows_count)
    offsets = jnp.where(inside, relative - relative // share * share, 0)
    owner_hot = owners[:, None] == lax.broadcasted_iota(jnp.int32, (count_pts, rows_count), 1)
    earlier = lax.broadcasted_iota(jnp.int32, (count_pts, count_pts), 1) < lax.broadcasted_iota(
        jnp.int32, (count_pts, count_pts), 0
    )
    before = jnp.dot(earlier.astype(BF16), owner_hot.astype(BF16), preferred_element_type=F32)
    ranking = jnp.sum(jnp.where(owner_hot, before, 0.0), axis=1).astype(jnp.int32)
    slot_index = jnp.where(inside, owners * capacity + ranking, -1)
    placing = (
        lax.broadcasted_iota(jnp.int32, (rows_count * capacity, count_pts), 0)
        == slot_index[None, :]
    )
    outgoing = jnp.dot(placing.astype(BF16), points, preferred_element_type=F32).astype(BF16)
    labels = (jnp.sum(jnp.where(placing, offsets[None, :] + 1, 0), axis=1) - 1).astype(BF16)
    arrived = lax.all_to_all(outgoing, "rows", split_axis=0, concat_axis=0, tiled=True)
    arrived_labels = lax.all_to_all(labels, "rows", split_axis=0, concat_axis=0, tiled=True)
    chosen = (
        lax.broadcasted_iota(jnp.int32, (share, arrived.shape[0]), 0)
        == arrived_labels.astype(jnp.int32)[None, :]
    )
    sums = jnp.dot(chosen.astype(BF16), arrived, preferred_element_type=F32)
    counts = jnp.sum(chosen.astype(F32), axis=1)
    piece = ((sums + own.astype(F32)) / (counts[:, None] + 1.0)).astype(BF16)
    updated = lax.all_gather(piece, "rows", axis=0, tiled=True)
    second = smallest(points, pnorm, updated)
    return block_min(jnp.stack([first, second])), updated


def fits(rows_count, share, capacity, count, width, blocksize):
    return (
        rows_count >= 8
        and rows_count & (rows_count - 1) == 0
        and share % 128 == 0
        and share <= 256
        and capacity % 16 == 0
        and count % 128 == 0
        and width % 128 == 0
        and blocksize % 256 == 0
    )


def per_device(points, centroids, assign):
    rows_count = lax.axis_size("rows")
    share = centroids.shape[0] // rows_count
    groups = rows_count * lax.axis_size("cent")
    capacity = max(2, 2 * points.shape[0] // groups)
    good = fits(rows_count, share, capacity, *points.shape, centroids.shape[0])
    if not good:
        return plain(points, centroids, assign, share, capacity)
    return halves(points, centroids, assign, share, capacity)


def solution(mesh):
    return jax.shard_map(
        per_device,
        mesh=mesh,
        in_specs=(P("rows", None), P("cent", None), P("rows")),
        out_specs=(P(None, "rows"), P("cent", None)),
        check_vma=False,
    )
```

```python
import functools

import jax
import jax.numpy as jnp
from jax import lax
from jax.experimental import pallas as pl
from jax.experimental.pallas import tpu as pltpu
from jax.sharding import PartitionSpec as P


F32 = jnp.float32
BF16 = jnp.bfloat16
VMEM = pl.BlockSpec(memory_space=pltpu.VMEM)
ANY = pl.BlockSpec(memory_space=pl.ANY)
HBM = pl.BlockSpec(memory_space=pltpu.HBM)
LIMIT = 24 * 1024 * 1024
WIDE = 58 * 1024 * 1024
LABEL_ROWS = 8


def swap(value, mask, axis="rows"):
    size = lax.axis_size(axis)
    return lax.ppermute(value, axis, [(i, i ^ mask) for i in range(size)])


def block_min(values):
    size = lax.axis_size("cent")
    if size & (size - 1):
        return lax.pmin(values, "cent")
    mask = 1
    while mask < size:
        values = jnp.minimum(values, swap(values, mask, "cent"))
        mask *= 2
    return values


def cost(flops, moved):
    return pl.CostEstimate(flops=int(flops), bytes_accessed=int(moved), transcendentals=0)


def params():
    return pltpu.CompilerParams(vmem_limit_bytes=LIMIT)


def rank_kernel(half, share, assign_ref, far_ref, near_ref, far_label_ref, near_label_ref):
    me, cent = lax.axis_index("rows"), lax.axis_index("cent")
    count = assign_ref.shape[1]
    seg = 128
    upper = jnp.where(
        lax.broadcasted_iota(jnp.int32, (seg, seg), 0)
        < lax.broadcasted_iota(jnp.int32, (seg, seg), 1),
        1.0,
        0.0,
    ).astype(BF16)
    low = lax.rem(me, half) ^ lax.broadcasted_iota(jnp.int32, (half, count), 0)
    for side, rank_ref, label_ref in (
        (1 - me // half, far_ref, far_label_ref),
        (me // half, near_ref, near_label_ref),
    ):
        within = assign_ref[...] - (cent * 2 * half + side * half + low) * share
        hot = (within >= 0) & (within < share)
        ones = jnp.where(hot, 1.0, 0.0).astype(F32)
        total = jnp.zeros((half, 1), F32)
        before = []
        for start in range(0, count, seg):
            piece = ones[:, start : start + seg]
            before.append(jnp.dot(piece.astype(BF16), upper, preferred_element_type=F32) + total)
            total = total + jnp.sum(piece, axis=1, keepdims=True)
        rank_ref[...] = jnp.where(hot, jnp.concatenate(before, axis=1), -1.0)
        label = jnp.sum(jnp.where(hot, within + 1, 0).astype(F32), axis=0, keepdims=True)
        label_ref[...] = jnp.transpose(jnp.broadcast_to(label, (8, count))).astype(BF16)


def ranks(assign_row, half, share):
    count = assign_row.shape[1]
    rank = jax.ShapeDtypeStruct((half, count), F32)
    label = jax.ShapeDtypeStruct((count, 8), BF16)
    return pl.pallas_call(
        functools.partial(rank_kernel, half, share),
        out_shape=[rank, rank, label, label],
        in_specs=[VMEM],
        out_specs=[VMEM] * 4,
        compiler_params=params(),
        cost_estimate=cost(2e9, 64 * count),
        name="ranks",
    )(assign_row)


def place_kernel(masks, capacity, rank_ref, label_ref, points_ref, *outs):
    count = points_ref.shape[0]
    slots = lax.broadcasted_iota(jnp.int32, (capacity, count), 0).astype(F32)
    placing = jnp.concatenate(
        [
            jnp.where(slots == rank_ref[m : m + 1, :], 1.0, 0.0).astype(BF16)
            for m in masks
        ],
        axis=0,
    )
    placed = jnp.dot(placing, points_ref[...], preferred_element_type=F32).astype(BF16)
    labels = jnp.dot(placing, label_ref[...], preferred_element_type=F32)
    labels = (jnp.transpose(labels) - 1.0).astype(BF16)
    for m in range(len(masks)):
        outs[m][:capacity, :] = placed[m * capacity : (m + 1) * capacity]
        outs[m][capacity:, :] = jnp.zeros((LABEL_ROWS, outs[m].shape[1]), BF16)
        outs[m][capacity:, :capacity] = labels[:, m * capacity : (m + 1) * capacity]


def place(rank, label, points, capacity, masks):
    half = len(masks)
    count, width = points.shape
    block = jax.ShapeDtypeStruct((capacity + LABEL_ROWS, width), BF16)
    blocks = pl.pallas_call(
        functools.partial(place_kernel, masks, capacity),
        out_shape=[block] * half,
        in_specs=[VMEM] * 3,
        out_specs=[VMEM] * half,
        compiler_params=params(),
        cost_estimate=cost(2 * half * capacity * count * width, 4 * count * width),
    )(rank, label, points)
    return dict(zip(masks, blocks, strict=True))


def sum_kernel(share, capacity, *refs):
    blocks, sums_ref, counts_ref = refs[:-2], refs[-2], refs[-1]
    labels = jnp.concatenate(
        [r[capacity:, :capacity].astype(F32)[:1] for r in blocks], axis=1
    )
    chosen = jnp.where(
        lax.broadcasted_iota(jnp.int32, (share, labels.shape[1]), 0).astype(F32) == labels, 1.0, 0.0
    ).astype(F32)
    rows = jnp.concatenate([r[:capacity, :] for r in blocks], axis=0)
    sums_ref[...] = jnp.dot(chosen.astype(BF16), rows, preferred_element_type=F32)
    counts = jnp.broadcast_to(jnp.sum(chosen, axis=1, keepdims=True), (share, 8))
    counts_ref[...] = jnp.transpose(counts)


def add_up(blocks, share, capacity):
    width = blocks[0].shape[1]
    return pl.pallas_call(
        functools.partial(sum_kernel, share, capacity),
        out_shape=[jax.ShapeDtypeStruct((share, width), F32), jax.ShapeDtypeStruct((8, share), F32)],
        in_specs=[VMEM] * len(blocks),
        out_specs=[VMEM, VMEM],
        compiler_params=params(),
        cost_estimate=cost(2 * share * len(blocks) * capacity * width, 3 * share * width * 4),
    )(*blocks)


def renew_kernel(sums_ref, counts_ref, far_sums_ref, far_counts_ref, own_ref, out_ref):
    counts = jnp.transpose(counts_ref[...] + far_counts_ref[...])[:, :1]
    total = sums_ref[...] + far_sums_ref[...] + own_ref[...].astype(F32)
    out_ref[...] = (total / (counts + 1.0)).astype(BF16)


def renew(sums, counts, far_sums, far_counts, own):
    return pl.pallas_call(
        renew_kernel,
        out_shape=jax.ShapeDtypeStruct(own.shape, BF16),
        in_specs=[VMEM] * 5,
        out_specs=VMEM,
        compiler_params=params(),
        cost_estimate=cost(4 * own.size, 14 * own.size),
        name="renew",
    )(sums, counts, far_sums, far_counts, own)


def lowest(cents, columns):
    wide = cents.astype(F32)
    norms = jnp.sum(wide * wide, axis=1, keepdims=True)
    scores = norms - 2.0 * jnp.dot(cents, columns, preferred_element_type=F32)
    return jnp.min(scores.reshape(-1, 8, scores.shape[1]), axis=0)


def first_kernel(cents_ref, columns_ref, out_ref):
    found = lowest(cents_ref[...], columns_ref[...])

    @pl.when(pl.program_id(0) == 0)
    def _():
        out_ref[...] = found

    @pl.when(pl.program_id(0) > 0)
    def _():
        out_ref[...] = jnp.minimum(out_ref[...], found)


def first_lowest(cents, columns):
    count, width = cents.shape
    step = 512 if count % 512 == 0 else 256
    out = jax.ShapeDtypeStruct((8, columns.shape[1]), F32)
    return pl.pallas_call(
        first_kernel,
        grid=(count // step,),
        out_shape=out,
        in_specs=[pl.BlockSpec((step, width), lambda i: (i, 0)), VMEM],
        out_specs=pl.BlockSpec(out.shape, lambda i: (0, 0)),
        compiler_params=pltpu.CompilerParams(vmem_limit_bytes=WIDE),
        cost_estimate=cost(2 * cents.size * columns.shape[1], 2 * cents.size),
        name="first_lowest",
    )(cents, columns)


def arrive_kernel(share, places, fresh, *refs):
    count = len(places)
    pieces, columns_ref = refs[:count], refs[count]
    rest = refs[count + 1 :] if fresh else refs[count + 3 :]
    running_out, whole_out, sems = rest
    me = lax.axis_index("rows")
    copies = []
    for i, ((mask, row), ref) in enumerate(zip(places, pieces, strict=True)):
        start = pl.multiple_of((me ^ mask) * share + row, ref.shape[0])
        copy = pltpu.make_async_copy(
            ref, whole_out.at[pl.ds(start, ref.shape[0])], sems.at[i]
        )
        copy.start()
        copies.append(copy)
    found = lowest(jnp.concatenate([r[...] for r in pieces], axis=0), columns_ref[...])
    running_out[...] = found if fresh else jnp.minimum(refs[count + 1][...], found)
    for copy in copies:
        copy.wait()


def low_kernel(*refs):
    pieces, (columns_ref, running_ref, out_ref) = refs[:-3], refs[-3:]
    found = lowest(jnp.concatenate([r[...] for r in pieces], axis=0), columns_ref[...])
    out_ref[...] = jnp.minimum(running_ref[...], found)


def write_kernel(share, places, *refs):
    count = len(places)
    pieces, (whole_out, held, in_sems, out_sems) = refs[:count], refs[count + 1 :]
    me = lax.axis_index("rows")
    moves, at = [], 0
    for i, ((mask, row), ref) in enumerate(zip(places, pieces, strict=True)):
        rows = ref.shape[0]
        slot = held.at[pl.ds(at, rows)]
        start = pl.multiple_of((me ^ mask) * share + row, rows)
        inward = pltpu.make_async_copy(ref, slot, in_sems.at[i])
        outward = pltpu.make_async_copy(slot, whole_out.at[pl.ds(start, rows)], out_sems.at[i])
        inward.start()
        moves.append((inward, outward))
        at += rows
    for inward, outward in moves:
        inward.wait()
        outward.start()
    for _, outward in moves:
        outward.wait()


def write(pieces, whole, share):
    places = [(mask, row) for mask, row, _ in pieces]
    operands = [array for _, _, array in pieces]
    rows, width = sum(o.shape[0] for o in operands), operands[0].shape[1]
    return pl.pallas_call(
        functools.partial(write_kernel, share, places),
        out_shape=jax.ShapeDtypeStruct(whole.shape, whole.dtype),
        in_specs=[ANY] * (len(operands) + 1),
        out_specs=ANY,
        scratch_shapes=[
            pltpu.VMEM((rows, width), BF16),
            pltpu.SemaphoreType.DMA((len(places),)),
            pltpu.SemaphoreType.DMA((len(places),)),
        ],
        input_output_aliases={len(operands): 0},
        compiler_params=params(),
        cost_estimate=cost(rows * width, 4 * rows * width),
        name="write_last",
    )(*operands, whole)


def arrive(pieces, columns, running, whole, total, share, writes=True):
    places = [(mask, row) for mask, row, _ in pieces]
    operands = [array for _, _, array in pieces]
    rows, width = sum(o.shape[0] for o in operands), operands[0].shape[1]
    fresh = running is None
    if not writes:
        return pl.pallas_call(
            low_kernel,
            out_shape=jax.ShapeDtypeStruct((8, columns.shape[1]), F32),
            in_specs=[VMEM] * (len(operands) + 2),
            out_specs=VMEM,
            compiler_params=params(),
            cost_estimate=cost(2 * rows * width * columns.shape[1], 2 * rows * width),
        )(*operands, columns, running), whole
    operands += [columns]
    specs = [VMEM] * len(operands)
    aliases = {}
    if not fresh:
        aliases = {len(operands) + 1: 1}
        operands += [running, whole]
        specs += [VMEM, ANY]
    return pl.pallas_call(
        functools.partial(arrive_kernel, share, places, fresh),
        out_shape=[
            jax.ShapeDtypeStruct((8, columns.shape[1]), F32),
            jax.ShapeDtypeStruct((total, width), BF16),
        ],
        in_specs=specs,
        out_specs=[VMEM, ANY],
        scratch_shapes=[pltpu.SemaphoreType.DMA((len(places),))],
        input_output_aliases=aliases,
        compiler_params=params(),
        cost_estimate=cost(2 * rows * width * columns.shape[1], 4 * rows * width),
    )(*operands)


def halves(points, centroids, assign, share, capacity):
    rows_count = lax.axis_size("rows")
    half = rows_count // 2
    me = lax.axis_index("rows")
    total = rows_count * share
    own = lax.dynamic_slice_in_dim(centroids, me * share, share, 0)
    assign_row = assign.reshape(1, -1)

    far_rank, near_rank, far_label, near_label = ranks(assign_row, half, share)
    powers = [m for m in range(half) if m and m & (m - 1) == 0]
    others = [m for m in range(half) if m not in powers]
    far = place(far_rank, far_label, points, capacity, powers)
    far |= place(far_rank, far_label, points, capacity, others)
    far = [far[0]] + [swap(far[m], m) for m in range(1, half)]
    early = [7, 6, 5] if half == 8 else [half - 1]
    rest = [m for m in range(half) if m not in early]
    near = place(near_rank, near_label, points, capacity, early)
    near |= place(near_rank, near_label, points, capacity, rest)
    near = [near[0]] + [swap(near[m], m) for m in range(1, half)]
    far_sums, far_counts = add_up(far, share, capacity)
    near[1], late = lax.optimization_barrier((near[1], points))
    far_sums = swap(far_sums, half)
    far_counts = swap(far_counts, half)
    columns = jnp.transpose(late)
    first = first_lowest(centroids, columns)
    near_sums, near_counts = add_up(near, share, capacity)
    pnorm = jnp.sum(jnp.square(late.astype(F32)), axis=1)
    first, pnorm, own, far_sums = lax.optimization_barrier((first, pnorm, own, far_sums))
    piece = renew(near_sums, near_counts, far_sums, far_counts, own)

    running, whole = None, None
    columns_count = rows_count // 4
    sets, corners = [], []
    for k in range(columns_count):
        one = piece if k == 0 else swap(piece, 4 * k)
        one_y = swap(one, 2)
        one_x = swap(one, 1)
        corner = swap(one_y, 1) if k % 2 == 0 else swap(one_x, 2)
        m = 4 * k
        sets.append([(m, 0, one), (m ^ 1, 0, one_x), (m ^ 2, 0, one_y)])
        corners.append((m ^ 3, 0, corner))
    for name, group in groups_of(columns_count):
        members = [p for k in group for p in sets[k]] if name == "set" else []
        if name == "set":
            members += [corners[k] for k in group]
            if group[0] == columns_count - 3:
                members += [sets[k][0] for k in range(columns_count - 2, columns_count)]
        elif name == "sides":
            members = [p for k in group for p in sets[k][1:]]
        else:
            members = [corners[k] for k in group]
        running, whole = arrive(members, columns, running, whole, total, share, name != "last")
    whole = write([corners[k] for k in group], whole, share)
    both = jnp.stack([jnp.min(first, axis=0), jnp.min(running, axis=0)])
    nearest = block_min((pnorm[None, :] + both) / points.shape[1])
    return nearest, whole


def groups_of(columns_count):
    early = [("set", (k,)) for k in range(columns_count - 2)]
    late = (columns_count - 2, columns_count - 1)
    return early + [("sides", late), ("last", late)]


def smallest(points, pnorm, cents):
    cnorm = jnp.sum(jnp.square(cents.astype(F32)), axis=1)
    dots = lax.dot_general(points, cents, (((1,), (1,)), ((), ())), preferred_element_type=F32)
    return jnp.min((pnorm[:, None] - 2.0 * dots + cnorm[None, :]) / points.shape[1], axis=1)


def plain(points, centroids, assign, share, capacity):
    blocksize = centroids.shape[0]
    count_pts = points.shape[0]
    pnorm = jnp.sum(jnp.square(points.astype(F32)), axis=1)
    first = smallest(points, pnorm, centroids)
    relative = assign - lax.axis_index("cent") * blocksize
    own = lax.dynamic_slice_in_dim(centroids, lax.axis_index("rows") * share, share, 0)
    rows_count = lax.axis_size("rows")
    inside = (relative >= 0) & (relative < blocksize)
    owners = jnp.where(inside, relative // share, rows_count)
    offsets = jnp.where(inside, relative - relative // share * share, 0)
    owner_hot = owners[:, None] == lax.broadcasted_iota(jnp.int32, (count_pts, rows_count), 1)
    earlier = lax.broadcasted_iota(jnp.int32, (count_pts, count_pts), 1) < lax.broadcasted_iota(
        jnp.int32, (count_pts, count_pts), 0
    )
    before = jnp.dot(earlier.astype(BF16), owner_hot.astype(BF16), preferred_element_type=F32)
    ranking = jnp.sum(jnp.where(owner_hot, before, 0.0), axis=1).astype(jnp.int32)
    slot_index = jnp.where(inside, owners * capacity + ranking, -1)
    placing = (
        lax.broadcasted_iota(jnp.int32, (rows_count * capacity, count_pts), 0)
        == slot_index[None, :]
    )
    outgoing = jnp.dot(placing.astype(BF16), points, preferred_element_type=F32).astype(BF16)
    labels = (jnp.sum(jnp.where(placing, offsets[None, :] + 1, 0), axis=1) - 1).astype(BF16)
    arrived = lax.all_to_all(outgoing, "rows", split_axis=0, concat_axis=0, tiled=True)
    arrived_labels = lax.all_to_all(labels, "rows", split_axis=0, concat_axis=0, tiled=True)
    chosen = (
        lax.broadcasted_iota(jnp.int32, (share, arrived.shape[0]), 0)
        == arrived_labels.astype(jnp.int32)[None, :]
    )
    sums = jnp.dot(chosen.astype(BF16), arrived, preferred_element_type=F32)
    counts = jnp.sum(chosen.astype(F32), axis=1)
    piece = ((sums + own.astype(F32)) / (counts[:, None] + 1.0)).astype(BF16)
    updated = lax.all_gather(piece, "rows", axis=0, tiled=True)
    second = smallest(points, pnorm, updated)
    return block_min(jnp.stack([first, second])), updated


def fits(rows_count, share, capacity, count, width, blocksize):
    return (
        rows_count >= 8
        and rows_count & (rows_count - 1) == 0
        and share % 128 == 0
        and share <= 256
        and capacity % 16 == 0
        and count % 128 == 0
        and width % 128 == 0
        and blocksize % 256 == 0
    )


def per_device(points, centroids, assign):
    rows_count = lax.axis_size("rows")
    share = centroids.shape[0] // rows_count
    groups = rows_count * lax.axis_size("cent")
    capacity = max(2, 2 * points.shape[0] // groups)
    good = fits(rows_count, share, capacity, *points.shape, centroids.shape[0])
    if not good:
        return plain(points, centroids, assign, share, capacity)
    return halves(points, centroids, assign, share, capacity)


def solution(mesh):
    return jax.shard_map(
        per_device,
        mesh=mesh,
        in_specs=(P("rows", None), P("cent", None), P("rows")),
        out_specs=(P(None, "rows"), P("cent", None)),
        check_vma=False,
    )
```
